32 devices in a mesh: dp: 1 (over z), tp: 32 (over y, x, core).
Axes of the slice: x: 4, y: 4, z: 1, core: 2. Of those that a mesh axis runs over, the one named last changes fastest.
The devices are a block of a 4x4x8 slice.
Arguments:
- hidden: bfloat16 [512, 4096], P('dp')
- w_gate: bfloat16 [4096, 11008], P(None, 'tp')
- w_up: bfloat16 [4096, 11008], P(None, 'tp')
- w_down: bfloat16 [11008, 4096], P('tp')
- norm_gain: float32 [4096], replicated
- w_vocab: bfloat16 [4096, 32000], P(None, 'tp')
- temperature: float32 [512], P('dp')
- target: int32 [512], P('dp')
Outputs:
- output 1: float32 [512], P('dp')
- output 2: float32 [512], P('dp')
- output 3: float32 [512], P('dp')
- output 4: bfloat16 [512, 32000], P('dp')
All inputs are finite; a program needn't handle non-finite values.
Results may differ from the reference program's by a relative error of at most 0.00463344.
Values are sent between devices in bfloat16 or wider.
A program may use at most 768 MiB of HBM per device.

```python
import jax
import jax.numpy as jnp
from jax import lax

MODEL_DIM = 4096
FF_DIM = 11008
VOCAB_SIZE = 32000
BATCH_ROWS = 512
ROW_BLOCK = min(32, BATCH_ROWS)
NORM_EPS = 1e-6


def setup_inputs(seed: int = 0, part: int = 0) -> dict:
    shared_keys = jax.random.split(jax.random.key(seed), 5)
    part_keys = jax.random.split(jax.random.fold_in(jax.random.key(seed + 1), part), 3)
    hidden = jax.random.normal(part_keys[0], (BATCH_ROWS, MODEL_DIM), jnp.float32)
    w_gate = jax.random.normal(shared_keys[0], (MODEL_DIM, FF_DIM), jnp.float32) * MODEL_DIM ** -0.5
    w_up = jax.random.normal(shared_keys[1], (MODEL_DIM, FF_DIM), jnp.float32) * MODEL_DIM ** -0.5
    w_down = jax.random.normal(shared_keys[2], (FF_DIM, MODEL_DIM), jnp.float32) * (2.0 * FF_DIM ** -0.5)
    norm_gain = jax.random.uniform(shared_keys[3], (MODEL_DIM,), jnp.float32, 0.5, 1.5)
    w_vocab = jax.random.normal(shared_keys[4], (MODEL_DIM, VOCAB_SIZE), jnp.float32) * (1.5 * MODEL_DIM ** -0.5)
    temperature = jax.random.uniform(part_keys[1], (BATCH_ROWS,), jnp.float32, 0.5, 2.0)
    target = jax.random.randint(part_keys[2], (BATCH_ROWS,), 0, VOCAB_SIZE, jnp.int32)
    return {
        "hidden": hidden.astype(jnp.bfloat16),
        "w_gate": w_gate.astype(jnp.bfloat16),
        "w_up": w_up.astype(jnp.bfloat16),
        "w_down": w_down.astype(jnp.bfloat16),
        "norm_gain": norm_gain,
        "w_vocab": w_vocab.astype(jnp.bfloat16),
        "temperature": temperature,
        "target": target,
    }


def reference(hidden, w_gate, w_up, w_down, norm_gain, w_vocab, temperature, target):
    block_count = hidden.shape[0] // ROW_BLOCK
    hidden_blocks = hidden.reshape(block_count, ROW_BLOCK, hidden.shape[1])
    temp_blocks = temperature.reshape(block_count, ROW_BLOCK)
    target_blocks = target.reshape(block_count, ROW_BLOCK)
    vocab_ids = jnp.arange(w_vocab.shape[1], dtype=jnp.int32)

    def one_block(block):
        hidden_rows, temp_rows, target_rows = block
        gate_pre = jnp.dot(hidden_rows, w_gate, preferred_element_type=jnp.float32)
        up_pre = jnp.dot(hidden_rows, w_up, preferred_element_type=jnp.float32)
        hidden_act = (jax.nn.silu(gate_pre) * up_pre).astype(jnp.bfloat16)
        mlp_out = jnp.dot(hidden_act, w_down, preferred_element_type=jnp.float32)
        residual = hidden_rows.astype(jnp.float32) + mlp_out
        inv_rms = lax.rsqrt(jnp.mean(residual * residual, axis=-1, keepdims=True) + NORM_EPS)
        normed = (norm_gain * residual * inv_rms).astype(jnp.bfloat16)
        logits = jnp.dot(normed, w_vocab, preferred_element_type=jnp.float32) / temp_rows[:, None]
        row_max = jnp.max(logits, axis=-1, keepdims=True)
        shifted = jnp.exp(logits - row_max)
        sum_exp = jnp.sum(shifted, axis=-1)
        log_norm = row_max[:, 0] + jnp.log(sum_exp)
        entropy = log_norm - jnp.sum(shifted * logits, axis=-1) / sum_exp
        target_logit = jnp.sum(jnp.where(vocab_ids[None, :] == target_rows[:, None], logits, 0.0), axis=-1)
        log_probs = (logits - log_norm[:, None]).astype(jnp.bfloat16)
        return log_norm, entropy, target_logit - log_norm, log_probs

    log_norm, entropy, target_logp, log_probs = lax.map(one_block, (hidden_blocks, temp_blocks, target_blocks))
    return (
        log_norm.reshape(-1),
        entropy.reshape(-1),
        target_logp.reshape(-1),
        log_probs.reshape(-1, w_vocab.shape[1]),
    )
```

```python
import functools
import math

import jax
import jax.numpy as jnp
from jax import lax
from jax.experimental import pallas as pl
from jax.experimental.pallas import tpu as pltpu
from jax.sharding import PartitionSpec as P

NORM_EPS = 1e-6
MESH = pl.DeviceIdType.MESH
NT = (((1,), (1,)), ((), ()))
PIECE = 1024
CHUNK = 256
SUB = 64


def place(side):
    me = lax.axis_index("tp")
    c = lax.rem(me, 2)
    chip = lax.div(me, 2)
    x, y = lax.rem(chip, side), lax.div(chip, side)
    i = x * (1 - c) + y * c
    j = y * (1 - c) + x * c
    s1 = 2 + (2 * side - 2) * c
    s2 = 2 * side - (2 * side - 2) * c

    def dev(a, b):
        return a * s1 + b * s2 + c

    nxt = lambda v: lax.rem(v + 1, side)
    prv = lambda v: lax.rem(v + side - 1, side)
    return me, c, i, j, dev(nxt(i), j), dev(prv(i), j), dev(i, nxt(j)), dev(i, prv(j)), me + 1 - 2 * c


def remote(src, dst, sems, k, to):
    return pltpu.make_async_remote_copy(
        src_ref=src, dst_ref=dst, send_sem=sems[0].at[k], recv_sem=sems[1].at[k],
        device_id={"tp": to}, device_id_type=MESH)


def sum_kernel(side, y_hbm, h_hbm, gain, x, Y, P0, T1a, T1b, T2a, T2b, H, lsem, ssem, rsem):
    me, c, i, j, R1, L1, R2, L2, PT = place(side)
    sems = (ssem, rsem)
    n1 = Y.shape[1] // 2
    n2 = n1 // side
    n3 = n2 // side
    pieces = Y.shape[0]
    half = pieces // 2

    base = pl.multiple_of(c * n1, n1)
    other = pl.multiple_of((1 - c) * n1, n1)
    row1 = lambda g: pl.multiple_of(c * n1 + g * n2, n2)
    row2 = lambda g: pl.multiple_of(c * n1 + i * n2 + g * n3, n3)
    mine = row2(j)

    loads = []
    for k, lo in enumerate((other, base)):
        for p in range(pieces):
            loads.append(pltpu.make_async_copy(
                y_hbm.at[pl.ds(lo, n1), pl.ds(p * PIECE, PIECE)], Y.at[p, pl.ds(lo, n1)], lsem.at[k * pieces + p]))
    for p in range(pieces):
        loads.append(pltpu.make_async_copy(
            h_hbm.at[pl.ds(mine, n3), pl.ds(p * PIECE, PIECE)], H.at[p], lsem.at[2 * pieces + p]))
    for cp in loads:
        cp.start()

    barrier = pltpu.get_barrier_semaphore()
    for to in (R1, L1, R2, L2, PT):
        pl.semaphore_signal(barrier, inc=1, device_id={"tp": to}, device_id_type=MESH)
    pl.semaphore_wait(barrier, 5)

    sent = []

    def start(cp):
        cp.start()
        sent.append(cp)
        return cp

    swaps = []
    for p in range(pieces):
        loads[p].wait()
        swaps.append(start(remote(Y.at[p, pl.ds(other, n1)], P0.at[p], sems, p, PT)))
    for cp in loads[pieces:]:
        cp.wait()

    f32 = lambda v: v.astype(jnp.float32)
    for p in range(pieces):
        swaps[p].wait_recv()
    nxt = lambda v: lax.rem(v + 1, side)
    prv = lambda v: lax.rem(v + side - 1, side)
    opp = lambda v: lax.rem(v + 2, side)

    def add_partner(g):
        def body(p, _):
            at = pl.ds(row1(g), n2)
            Y[p, at] = (f32(Y[p, at]) + f32(P0[p, pl.ds(pl.multiple_of(g * n2, n2), n2)])).astype(jnp.bfloat16)
            return 0
        lax.fori_loop(0, pieces, body, 0)

    def ring_sum(pos, row, n, R, L, Ta, Tb, k, prepare):
        prepare(opp(pos))
        lo, hi = pl.ds(0, half), pl.ds(half, half)
        far = pl.ds(row(opp(pos)), n)
        m0 = start(remote(Y.at[lo, far], Ta.at[0], sems, k, R))
        m1 = start(remote(Y.at[hi, far], Ta.at[1], sems, k + 1, L))
        prepare(nxt(pos))
        prepare(prv(pos))
        right, left = pl.ds(row(nxt(pos)), n), pl.ds(row(prv(pos)), n)
        m0.wait_recv()
        for p in range(half):
            Y[p, right] = (f32(Y[p, right]) + f32(Ta[0, p])).astype(jnp.bfloat16)
        m2 = start(remote(Y.at[:, right], Tb.at[0], sems, k + 2, R))
        m1.wait_recv()
        for p in range(half):
            Y[half + p, left] = (f32(Y[half + p, left]) + f32(Ta[1, p])).astype(jnp.bfloat16)
        m3 = start(remote(Y.at[:, left], Tb.at[1], sems, k + 3, L))
        prepare(pos)
        m2.wait_recv()
        m3.wait_recv()

    ring_sum(i, row1, n2, R1, L1, T1a, T1b, 4, add_partner)
    own = pl.ds(row1(i), n2)
    for p in range(pieces):
        Y[p, own] = (f32(Y[p, own]) + f32(T1b[0, p]) + f32(T1b[1, p])).astype(jnp.bfloat16)
    ring_sum(j, row2, n3, R2, L2, T2a, T2b, 8, lambda g: None)

    at = pl.ds(mine, n3)
    total = jnp.zeros((n3, 1), jnp.float32)
    rs = []
    for p in range(pieces):
        r = f32(H[p]) + (f32(Y[p, at]) + f32(T2b[0, p]) + f32(T2b[1, p]))
        rs.append(r)
        total += jnp.sum(r * r, axis=-1, keepdims=True)
    inv = lax.rsqrt(total / (pieces * PIECE) + NORM_EPS)
    for p in range(pieces):
        x[p, at] = (gain[0:1, p * PIECE:(p + 1) * PIECE] * rs[p] * inv).astype(jnp.bfloat16)

    def ring_gather(pos, row, n, R, L, k):
        lo, hi = pl.ds(0, half), pl.ds(half, half)
        own = x.at[:, pl.ds(row(pos), n)]
        left, right, far = row(prv(pos)), row(nxt(pos)), row(opp(pos))
        at = lambda r, ps=slice(None): x.at[ps, pl.ds(r, n)]
        start(remote(own, own, sems, k, R))
        start(remote(own, own, sems, k + 1, L))
        remote(at(left), at(left), sems, k, R).wait_recv()
        start(remote(at(left, lo), at(left, lo), sems, k + 2, R))
        remote(at(right), at(right), sems, k + 1, L).wait_recv()
        start(remote(at(right, hi), at(right, hi), sems, k + 3, L))
        yield left
        yield right
        remote(at(far, lo), at(far, lo), sems, k + 2, R).wait_recv()
        remote(at(far, hi), at(far, hi), sems, k + 3, L).wait_recv()
        yield far

    for _ in ring_gather(j, row2, n3, R2, L2, 12):
        pass
    k = 20
    line = x.at[:, pl.ds(row1(i), n2)]
    start(remote(line, line, sems, k, PT))
    for r in ring_gather(i, row1, n2, R1, L1, 16):
        k += 1
        line = x.at[:, pl.ds(r, n2)]
        start(remote(line, line, sems, k, PT))
    ip = j
    rowp = lambda g: pl.multiple_of((1 - c) * n1 + g * n2, n2)
    for k, g in enumerate((ip, prv(ip), nxt(ip), opp(ip))):
        line = x.at[:, pl.ds(rowp(g), n2)]
        remote(line, line, sems, 20 + k, PT).wait_recv()
    for cp in sent:
        cp.wait_send()


def head_kernel(side, n_dev, v_loc, x, wv_hbm, temp, target, G, out, WV, LT, LP, ST, wsem, ssem, rsem, stsem, strsem):
    me, c, i, j, R1, L1, R2, L2, PT = place(side)
    rows = x.shape[1]
    pieces = x.shape[0]
    vpad = WV.shape[1]
    chunks = rows // CHUNK
    subs = rows // SUB
    nxt = lambda v: lax.rem(v + 1, side)
    prv = lambda v: lax.rem(v + side - 1, side)
    opp = lambda v: lax.rem(v + 2, side)

    wloads = [pltpu.make_async_copy(
        wv_hbm.at[:, pl.ds(p * PIECE, PIECE)], WV.at[p, pl.ds(0, v_loc)], wsem.at[p]) for p in range(pieces)]
    for cp in wloads:
        cp.start()
    barrier = pltpu.get_barrier_semaphore()

    def greet(t, _):
        to = lax.rem(me + 1 + t, n_dev)
        pl.semaphore_signal(barrier, inc=1, device_id={"tp": to}, device_id_type=MESH)
        return 0
    lax.fori_loop(0, n_dev - 1, greet, 0)
    for p in range(pieces):
        WV[p, v_loc:] = jnp.zeros((vpad - v_loc, PIECE), WV.dtype)
    for cp in wloads:
        cp.wait()

    vid = lax.broadcasted_iota(jnp.int32, (vpad, CHUNK), 0)
    for k in range(chunks):
        at = pl.ds(k * CHUNK, CHUNK)
        acc = lax.dot_general(WV[0], x[0, at], NT, preferred_element_type=jnp.float32)
        for p in range(1, pieces):
            acc += lax.dot_general(WV[p], x[p, at], NT, preferred_element_type=jnp.float32)
        l = acc / temp[0:1, k * CHUNK:(k + 1) * CHUNK]
        LT[k] = l
        real = vid < v_loc
        m = jnp.max(jnp.where(real, l, -jnp.inf), axis=0, keepdims=True)
        e = jnp.where(real, jnp.exp(l - m), 0.0)
        s = jnp.sum(e, axis=0, keepdims=True)
        w = jnp.sum(e * l, axis=0, keepdims=True)
        ids = target[0:1, k * CHUNK:(k + 1) * CHUNK] - me * v_loc
        t = jnp.sum(jnp.where((vid == ids) & real, l, 0.0), axis=0, keepdims=True)
        both = [v[:, h * 128:(h + 1) * 128] for h in range(CHUNK // 128) for v in (m, s, w, t)]
        ST[k, me] = jnp.concatenate(both, axis=0)
        if k == 0:
            pl.semaphore_wait(barrier, n_dev - 1)

        def tell(t, _, k=k):
            to = lax.rem(me + 1 + t, n_dev)
            pltpu.make_async_remote_copy(
                src_ref=ST.at[k, me], dst_ref=ST.at[k, me], send_sem=stsem.at[k, t], recv_sem=strsem.at[k, t],
                device_id={"tp": to}, device_id_type=MESH).start()
            return 0
        lax.fori_loop(0, n_dev - 1, tell, 0)

    def heard(k, wait):
        def body(t, _):
            frm = lax.rem(me + n_dev - 1 - t, n_dev)
            cp = pltpu.make_async_remote_copy(
                src_ref=ST.at[k, me], dst_ref=ST.at[k, frm], send_sem=stsem.at[k, t], recv_sem=strsem.at[k, t],
                device_id={"tp": frm}, device_id_type=MESH)
            wait(cp)
            return 0
        lax.fori_loop(0, n_dev - 1, body, 0)

    sems = (ssem, rsem)
    sent = []

    def start(cp):
        cp.start()
        sent.append(cp)

    lo, hi = pl.ds(0, SUB // 2), pl.ds(SUB // 2, SUB // 2)

    def own(k):
        b = G.at[c, i, j, pl.ds(k * SUB, SUB)]
        start(remote(b, b, sems, 12 * k, R1))
        start(remote(b, b, sems, 12 * k + 1, L1))

    def blk(a, b, k, part=None):
        if part is None:
            return G.at[c, a, b, pl.ds(k * SUB, SUB)]
        return G.at[c, a, b, pl.ds(k * SUB + part * (SUB // 2), SUB // 2)]

    def first(k):
        left, right = prv(i), nxt(i)
        remote(blk(left, j, k), blk(left, j, k), sems, 12 * k, R1).wait_recv()
        b = blk(left, j, k, 0)
        start(remote(b, b, sems, 12 * k + 2, R1))
        remote(blk(right, j, k), blk(right, j, k), sems, 12 * k + 1, L1).wait_recv()
        b = blk(right, j, k, 1)
        start(remote(b, b, sems, 12 * k + 3, L1))

    def line(b, k, a0=0, na=side):
        return G.at[c, pl.ds(a0, na), b, pl.ds(k * SUB, SUB)]

    def second(k):
        far = opp(i)
        for part in range(2):
            b = blk(far, j, k, part)
            remote(b, b, sems, 12 * k + 2 + part, R1).wait_recv()
        b = line(j, k)
        start(remote(b, b, sems, 12 * k + 4, R2))
        start(remote(b, b, sems, 12 * k + 5, L2))
        start(remote(b, b, sems, 12 * k + 8, PT))

    def third(k):
        b = line(prv(j), k)
        remote(b, b, sems, 12 * k + 4, R2).wait_recv()
        b2 = line(prv(j), k, 0, side // 2)
        start(remote(b2, b2, sems, 12 * k + 6, R2))
        start(remote(b, b, sems, 12 * k + 9, PT))
        b = line(nxt(j), k)
        remote(b, b, sems, 12 * k + 5, L2).wait_recv()
        b2 = line(nxt(j), k, side // 2, side // 2)
        start(remote(b2, b2, sems, 12 * k + 7, L2))
        start(remote(b, b, sems, 12 * k + 10, PT))

    def fourth(k):
        for part in range(2):
            b = line(opp(j), k, part * (side // 2), side // 2)
            remote(b, b, sems, 12 * k + 6 + part, R2).wait_recv()
        b = line(opp(j), k)
        start(remote(b, b, sems, 12 * k + 11, PT))

    def last(k):
        jp = i
        for q, g in enumerate((jp, prv(jp), nxt(jp), opp(jp))):
            b = G.at[1 - c, :, g, pl.ds(k * SUB, SUB)]
            remote(b, b, sems, 12 * k + 8 + q, PT).wait_recv()

    per = CHUNK // SUB
    step = 0

    def advance(limit):
        nonlocal step
        while step < limit:
            own(step)
            for lag, act in ((1, first), (2, second), (3, third), (4, fourth), (5, last)):
                if step >= lag:
                    act(step - lag)
            step += 1

    for k in range(chunks):
        heard(k, lambda cp: cp.wait_recv())
        st = ST[k]
        for h in range(CHUNK // 128):
            b = 4 * h
            ms, ss, ws, ts = (st[:, b + q:b + q + 1, :] for q in range(4))
            m = jnp.max(ms, axis=0)
            f = jnp.exp(ms - m[None])
            s = jnp.sum(ss * f, axis=0)
            w = jnp.sum(ws * f, axis=0)
            t = jnp.sum(ts, axis=0)
            ln = m + jnp.log(s)
            cols = pl.ds(k * CHUNK + h * 128, 128)
            out[0:1, cols] = ln
            out[1:2, cols] = ln - w / s
            out[2:3, cols] = t - ln
            LP[...] = LT[k, :, h * 128:(h + 1) * 128] - ln

            def turn(q, _, k=k, h=h):
                v = pl.ds(pl.multiple_of(q * 128, 128), 128)
                G[c, i, j, pl.ds(k * CHUNK + h * 128, 128), v] = LP[v].T.astype(jnp.bfloat16)
                return 0
            lax.fori_loop(0, vpad // 128, turn, 0)
            advance(k * per + (h + 1) * 128 // SUB)
    for k in range(subs, subs + 5):
        for lag, act in ((1, first), (2, second), (3, third), (4, fourth), (5, last)):
            if lag <= k and k - lag < subs:
                act(k - lag)
    for k in range(chunks):
        heard(k, lambda cp: cp.wait_send())
    for cp in sent:
        cp.wait_send()


def layout_kernel(side, v_loc, g, o):
    r = pl.ds(pl.multiple_of(pl.program_id(0) * o.shape[0], o.shape[0]), o.shape[0])
    for fam in range(2):
        for a in range(side):
            for b in range(side):
                d = ((b * side + a) * 2) if fam == 0 else ((a * side + b) * 2 + 1)
                o[:, d * v_loc:(d + 1) * v_loc] = g[fam, a, b, r, 0:v_loc]


def solution(mesh):
    n_dev = mesh.shape["tp"]
    side = math.isqrt(n_dev // 2)

    def device_step(hidden, w_gate, w_up, w_down, norm_gain, w_vocab, temperature, target):
        rows, d = hidden.shape
        v_loc = w_vocab.shape[1]
        pieces = d // PIECE
        vpad = -(-v_loc // 128) * 128
        gate_pre = jnp.dot(hidden, w_gate, preferred_element_type=jnp.float32)
        up_pre = jnp.dot(hidden, w_up, preferred_element_type=jnp.float32)
        hidden_act = (jax.nn.silu(gate_pre) * up_pre).astype(jnp.bfloat16)
        part_sum = jnp.dot(hidden_act, w_down, preferred_element_type=jnp.float32).astype(jnp.bfloat16)

        n1 = rows // 2
        n2, n3 = n1 // side, n1 // side // side
        vm = pl.BlockSpec(memory_space=pltpu.VMEM)
        hbm = pl.BlockSpec(memory_space=pl.ANY)
        bf = jnp.bfloat16
        x = pl.pallas_call(
            functools.partial(sum_kernel, side),
            out_shape=pltpu.VMEM((pieces, rows, PIECE), bf),
            in_specs=[hbm, hbm, vm],
            out_specs=vm,
            scratch_shapes=[
                pltpu.VMEM((pieces, rows, PIECE), bf),
                pltpu.VMEM((pieces, n1, PIECE), bf),
                pltpu.VMEM((2, pieces // 2, n2, PIECE), bf),
                pltpu.VMEM((2, pieces, n2, PIECE), bf),
                pltpu.VMEM((2, pieces // 2, n3, PIECE), bf),
                pltpu.VMEM((2, pieces, n3, PIECE), bf),
                pltpu.VMEM((pieces, n3, PIECE), bf),
                pltpu.SemaphoreType.DMA((3 * pieces,)),
                pltpu.SemaphoreType.DMA((24,)),
                pltpu.SemaphoreType.DMA((24,)),
            ],
            compiler_params=pltpu.CompilerParams(
                collective_id=0, has_side_effects=True, vmem_limit_bytes=20 << 20),
            name="sum_norm",
        )(part_sum, hidden, norm_gain.reshape(1, d))

        chunks, subs = rows // CHUNK, rows // SUB
        g, stats = pl.pallas_call(
            functools.partial(head_kernel, side, n_dev, v_loc),
            out_shape=(pltpu.VMEM((2, side, side, rows, vpad), bf), pltpu.VMEM((8, rows), jnp.float32)),
            in_specs=[vm, hbm, vm, vm],
            out_specs=(vm, vm),
            scratch_shapes=[
                pltpu.VMEM((pieces, vpad, PIECE), bf),
                pltpu.VMEM((chunks, vpad, CHUNK), jnp.float32),
                pltpu.VMEM((vpad, 128), jnp.float32),
                pltpu.VMEM((chunks, n_dev, 8, 128), jnp.float32),
                pltpu.SemaphoreType.DMA((pieces,)),
                pltpu.SemaphoreType.DMA((12 * subs,)),
                pltpu.SemaphoreType.DMA((12 * subs,)),
                pltpu.SemaphoreType.DMA((chunks, n_dev - 1)),
                pltpu.SemaphoreType.DMA((chunks, n_dev - 1)),
            ],
            compiler_params=pltpu.CompilerParams(
                collective_id=1, has_side_effects=True, vmem_limit_bytes=24 << 20),
            name="head",
        )(x, w_vocab.T, temperature.reshape(1, rows), target.reshape(1, rows))

        step = 32
        log_probs = pl.pallas_call(
            functools.partial(layout_kernel, side, v_loc),
            out_shape=jax.ShapeDtypeStruct((rows, n_dev * v_loc), bf),
            grid=(rows // step,),
            in_specs=[vm],
            out_specs=pl.BlockSpec((step, n_dev * v_loc), lambda s: (s, 0)),
            compiler_params=pltpu.CompilerParams(vmem_limit_bytes=16 << 20),
            name="layout",
        )(g)
        return stats[0], stats[1], stats[2], log_probs

    return jax.shard_map(
        device_step,
        mesh=mesh,
        in_specs=(P("dp", None), P(None, "tp"), P(None, "tp"), P("tp", None), P(None),
                  P(None, "tp"), P("dp"), P("dp")),
        out_specs=(P("dp"), P("dp"), P("dp"), P("dp", None)),
        check_vma=False,
    )
```

```python
import functools
import math

import jax
import jax.numpy as jnp
from jax import lax
from jax.experimental import pallas as pl
from jax.experimental.pallas import tpu as pltpu
from jax.sharding import PartitionSpec as P

NORM_EPS = 1e-6
MESH = pl.DeviceIdType.MESH
NT = (((1,), (1,)), ((), ()))
PIECE = 1024
CHUNK = 256
SUB = 128


def place(side):
    me = lax.axis_index("tp")
    c = lax.rem(me, 2)
    chip = lax.div(me, 2)
    x, y = lax.rem(chip, side), lax.div(chip, side)
    i = x * (1 - c) + y * c
    j = y * (1 - c) + x * c
    s1 = 2 + (2 * side - 2) * c
    s2 = 2 * side - (2 * side - 2) * c

    def dev(a, b):
        return a * s1 + b * s2 + c

    nxt = lambda v: lax.rem(v + 1, side)
    prv = lambda v: lax.rem(v + side - 1, side)
    return me, c, i, j, dev(nxt(i), j), dev(prv(i), j), dev(i, nxt(j)), dev(i, prv(j)), me + 1 - 2 * c


def remote(src, dst, sems, k, to):
    return pltpu.make_async_remote_copy(
        src_ref=src, dst_ref=dst, send_sem=sems[0].at[k], recv_sem=sems[1].at[k],
        device_id={"tp": to}, device_id_type=MESH)


def tail_kernel(side, n_dev, f_loc, v_loc, h_hbm, wg_hbm, wu_hbm, wd_hbm, gain, wv_hbm, temp, target, G, out,
                H, W, WD, X, WV, LT, LP, ST, lsem, ssem, rsem, gssem, grsem, stsem, strsem):
    me, c, i, j, R1, L1, R2, L2, PT = place(side)
    rows, d = H.shape
    vpad = WV.shape[0]
    fpad = WD.shape[0]
    pieces = d // PIECE
    half = pieces // 2
    chunks = rows // CHUNK
    subs = rows // SUB
    n1 = CHUNK // 2
    n2 = n1 // side
    n3 = n2 // side
    f32 = lambda v: v.astype(jnp.float32)
    bf16 = lambda v: v.astype(jnp.bfloat16)
    nxt = lambda v: lax.rem(v + 1, side)
    prv = lambda v: lax.rem(v + side - 1, side)
    opp = lambda v: lax.rem(v + 2, side)

    loads = {}

    def load(name, src, dst):
        cp = pltpu.make_async_copy(src, dst, lsem.at[len(loads)])
        cp.start()
        loads[name] = cp

    load("h0", h_hbm.at[pl.ds(0, CHUNK)], H.at[pl.ds(0, CHUNK)])
    load("wg", wg_hbm, W.at[pl.ds(0, f_loc)])
    load("wu", wu_hbm, W.at[pl.ds(fpad, f_loc)])
    load("wd", wd_hbm, WD.at[pl.ds(0, f_loc)])
    for b in range(1, chunks):
        load("h%d" % b, h_hbm.at[pl.ds(b * CHUNK, CHUNK)], H.at[pl.ds(b * CHUNK, CHUNK)])
    load("wv", wv_hbm, WV.at[pl.ds(0, v_loc)])

    barrier = pltpu.get_barrier_semaphore()

    def greet(t, _):
        to = lax.rem(me + 1 + t, n_dev)
        pl.semaphore_signal(barrier, inc=1, device_id={"tp": to}, device_id_type=MESH)
        return 0
    lax.fori_loop(0, n_dev - 1, greet, 0)
    W[f_loc:fpad] = jnp.zeros((fpad - f_loc, d), W.dtype)
    W[fpad + f_loc:] = jnp.zeros((fpad - f_loc, d), W.dtype)
    WD[f_loc:] = jnp.zeros((fpad - f_loc, d), WD.dtype)
    WV[v_loc:] = jnp.zeros((vpad - v_loc, d), WV.dtype)

    sent = []

    def start(cp):
        cp.start()
        sent.append(cp)
        return cp

    Y = G.at[0, 0]

    def mlp(b):
        gu = lax.dot_general(W[...], H[b * CHUNK:(b + 1) * CHUNK], NT, preferred_element_type=jnp.float32)
        g, u = gu[:fpad], gu[fpad:]
        a = bf16((g * lax.logistic(g) * u).T)
        if b == 0:
            loads["wd"].wait()
            pl.semaphore_wait(barrier, n_dev - 1)
        for p in range(pieces):
            Y[p, b * CHUNK:(b + 1) * CHUNK] = bf16(
                jnp.dot(a, WD[:, p * PIECE:(p + 1) * PIECE], preferred_element_type=jnp.float32))
            theirs = Y.at[p, pl.ds(pl.multiple_of(b * CHUNK + (1 - c) * n1, n1), n1)]
            start(remote(theirs, G.at[0, 1, p, pl.ds(b * n1, n1)], (ssem, rsem), 24 * b + p, PT))

    def chain(b):
        sems = (ssem, rsem)
        k0 = 24 * b
        P0 = G.at[0, 1]
        T = G.at[1, b]
        lo, hi, every = pl.ds(0, half), pl.ds(half, half), pl.ds(0, pieces)
        row1 = lambda g: pl.multiple_of(b * CHUNK + c * n1 + g * n2, n2)
        row2 = lambda g: pl.multiple_of(b * CHUNK + c * n1 + i * n2 + g * n3, n3)

        def add_partner(g):
            at = pl.ds(row1(g), n2)
            frm = pl.ds(pl.multiple_of(b * n1 + g * n2, n2), n2)
            for p in range(pieces):
                Y[p, at] = bf16(f32(Y[p, at]) + f32(P0[p, frm]))

        def ring_sum(pos, row, n, R, L, t0, k, prepare):
            ta, tl, tr = pl.ds(t0, n), pl.ds(t0 + n, n), pl.ds(t0 + 2 * n, n)
            prepare(opp(pos))
            far = pl.ds(row(opp(pos)), n)
            m0 = start(remote(Y.at[lo, far], T.at[lo, ta], sems, k, R))
            m1 = start(remote(Y.at[hi, far], T.at[hi, ta], sems, k + 1, L))
            prepare(nxt(pos))
            prepare(prv(pos))
            right, left = pl.ds(row(nxt(pos)), n), pl.ds(row(prv(pos)), n)
            yield
            m0.wait_recv()
            for p in range(half):
                Y[p, right] = bf16(f32(Y[p, right]) + f32(T[p, ta]))
            m2 = start(remote(Y.at[every, right], T.at[every, tl], sems, k + 2, R))
            m1.wait_recv()
            for p in range(half, pieces):
                Y[p, left] = bf16(f32(Y[p, left]) + f32(T[p, ta]))
            m3 = start(remote(Y.at[every, left], T.at[every, tr], sems, k + 3, L))
            prepare(pos)
            yield
            m2.wait_recv()
            m3.wait_recv()
            own = pl.ds(row(pos), n)
            for p in range(pieces):
                total = f32(Y[p, own]) + f32(T[p, tl]) + f32(T[p, tr])
                yield p, total

        def drive(steps, keep):
            for got in steps:
                if got is None:
                    yield
                else:
                    keep(*got)

        yield
        for p in range(pieces):
            box = G.at[0, 1, p, pl.ds(b * n1, n1)]
            remote(box, box, sems, k0 + p, PT).wait_recv()
        own1 = pl.ds(row1(i), n2)

        def keep1(p, total):
            Y[p, own1] = bf16(total)
        yield from drive(ring_sum(i, row1, n2, R1, L1, 0, k0 + 4, add_partner), keep1)
        sums = []
        yield from drive(ring_sum(j, row2, n3, R2, L2, 3 * n2, k0 + 8, lambda g: None), lambda p, t: sums.append(t))

        mine = pl.ds(row2(j), n3)
        square = jnp.zeros((n3, 1), jnp.float32)
        for p in range(pieces):
            sums[p] = f32(H[mine, p * PIECE:(p + 1) * PIECE]) + sums[p]
            square += jnp.sum(sums[p] * sums[p], axis=-1, keepdims=True)
        inv = lax.rsqrt(square / d + NORM_EPS)
        for p in range(pieces):
            cols = slice(p * PIECE, (p + 1) * PIECE)
            X[mine, cols] = bf16(gain[0:1, cols] * sums[p] * inv)

        left_half, right_half = pl.ds(0, d // 2), pl.ds(d // 2, d // 2)

        def ring_gather(pos, row, n, R, L, k):
            at = lambda r, cols=pl.ds(0, d): X.at[pl.ds(r, n), cols]
            own, left, right, far = row(pos), row(prv(pos)), row(nxt(pos)), row(opp(pos))
            start(remote(at(own), at(own), sems, k, R))
            start(remote(at(own), at(own), sems, k + 1, L))
            yield own
            yield
            remote(at(left), at(left), sems, k, R).wait_recv()
            start(remote(at(left, left_half), at(left, left_half), sems, k + 2, R))
            remote(at(right), at(right), sems, k + 1, L).wait_recv()
            start(remote(at(right, right_half), at(right, right_half), sems, k + 3, L))
            yield left
            yield right
            yield
            remote(at(far, left_half), at(far, left_half), sems, k + 2, R).wait_recv()
            remote(at(far, right_half), at(far, right_half), sems, k + 3, L).wait_recv()
            yield far

        for got in ring_gather(j, row2, n3, R2, L2, k0 + 12):
            if got is None:
                yield
        k = k0 + 20
        for got in ring_gather(i, row1, n2, R1, L1, k0 + 16):
            if got is None:
                yield
            else:
                line = X.at[pl.ds(got, n2)]
                start(remote(line, line, sems, k, PT))
                k += 1
        yield
        for q, g in enumerate((j, prv(j), nxt(j), opp(j))):
            line = X.at[pl.ds(pl.multiple_of(b * CHUNK + (1 - c) * n1 + g * n2, n2), n2)]
            remote(line, line, sems, k0 + 20 + q, PT).wait_recv()

    vid = lax.broadcasted_iota(jnp.int32, (vpad, CHUNK), 0)

    def logits(b):
        cols = slice(b * CHUNK, (b + 1) * CHUNK)
        l = lax.dot_general(WV[...], X[cols], NT, preferred_element_type=jnp.float32) / temp[0:1, cols]
        LT[b] = l
        real = vid < v_loc
        m = jnp.max(jnp.where(real, l, -jnp.inf), axis=0, keepdims=True)
        e = jnp.where(real, jnp.exp(l - m), 0.0)
        s = jnp.sum(e, axis=0, keepdims=True)
        w = jnp.sum(e * l, axis=0, keepdims=True)
        ids = target[0:1, cols] - me * v_loc
        t = jnp.sum(jnp.where((vid == ids) & real, l, 0.0), axis=0, keepdims=True)
        both = [v[:, h * 128:(h + 1) * 128] for h in range(CHUNK // 128) for v in (m, s, w, t)]
        ST[b, me] = jnp.concatenate(both, axis=0)

    def tell(b):
        def body(t, _):
            to = lax.rem(me + 1 + t, n_dev)
            pltpu.make_async_remote_copy(
                src_ref=ST.at[b, me], dst_ref=ST.at[b, me], send_sem=stsem.at[b, t], recv_sem=strsem.at[b, t],
                device_id={"tp": to}, device_id_type=MESH).start()
            return 0
        lax.fori_loop(0, n_dev - 1, body, 0)

    def heard(b, wait):
        def body(t, _):
            frm = lax.rem(me + n_dev - 1 - t, n_dev)
            cp = pltpu.make_async_remote_copy(
                src_ref=ST.at[b, me], dst_ref=ST.at[b, frm], send_sem=stsem.at[b, t], recv_sem=strsem.at[b, t],
                device_id={"tp": frm}, device_id_type=MESH)
            wait(cp)
            return 0
        lax.fori_loop(0, n_dev - 1, body, 0)

    sems = (gssem, grsem)

    def blk(a, b, k, part=None):
        if part is None:
            return G.at[c, a, b, pl.ds(k * SUB, SUB)]
        return G.at[c, a, b, pl.ds(k * SUB + part * (SUB // 2), SUB // 2)]

    def line(b, k, a0=0, na=side):
        return G.at[c, pl.ds(a0, na), b, pl.ds(k * SUB, SUB)]

    def combine(b):
        heard(b, lambda cp: cp.wait_recv())
        st = ST[b]
        for h in range(CHUNK // 128):
            ms, ss, ws, ts = (st[:, 4 * h + q:4 * h + q + 1, :] for q in range(4))
            m = jnp.max(ms, axis=0)
            f = jnp.exp(ms - m[None])
            s = jnp.sum(ss * f, axis=0)
            w = jnp.sum(ws * f, axis=0)
            t = jnp.sum(ts, axis=0)
            ln = m + jnp.log(s)
            cols = pl.ds(b * CHUNK + h * 128, 128)
            out[0:1, cols] = ln
            out[1:2, cols] = ln - w / s
            out[2:3, cols] = t - ln
            LP[...] = LT[b, :, h * 128:(h + 1) * 128] - ln

            def turn(q, _, h=h):
                v = pl.ds(pl.multiple_of(q * 128, 128), 128)
                G[c, i, j, pl.ds(b * CHUNK + h * 128, 128), v] = bf16(LP[v].T)
                return 0
            lax.fori_loop(0, vpad // 128, turn, 0)
            for k in range((b * CHUNK + h * 128) // SUB, (b * CHUNK + (h + 1) * 128) // SUB):
                own = blk(i, j, k)
                start(remote(own, own, sems, 12 * k, R1))
                start(remote(own, own, sems, 12 * k + 1, L1))

    def first(k):
        left, right = prv(i), nxt(i)
        remote(blk(left, j, k), blk(left, j, k), sems, 12 * k, R1).wait_recv()
        b = blk(left, j, k, 0)
        start(remote(b, b, sems, 12 * k + 2, R1))
        remote(blk(right, j, k), blk(right, j, k), sems, 12 * k + 1, L1).wait_recv()
        b = blk(right, j, k, 1)
        start(remote(b, b, sems, 12 * k + 3, L1))

    def second(k):
        for part in range(2):
            b = blk(opp(i), j, k, part)
            remote(b, b, sems, 12 * k + 2 + part, R1).wait_recv()
        b = line(j, k)
        start(remote(b, b, sems, 12 * k + 4, R2))
        start(remote(b, b, sems, 12 * k + 5, L2))
        start(remote(b, b, sems, 12 * k + 8, PT))

    def third(k):
        b = line(prv(j), k)
        remote(b, b, sems, 12 * k + 4, R2).wait_recv()
        b2 = line(prv(j), k, 0, side // 2)
        start(remote(b2, b2, sems, 12 * k + 6, R2))
        start(remote(b, b, sems, 12 * k + 9, PT))
        b = line(nxt(j), k)
        remote(b, b, sems, 12 * k + 5, L2).wait_recv()
        b2 = line(nxt(j), k, side // 2, side // 2)
        start(remote(b2, b2, sems, 12 * k + 7, L2))
        start(remote(b, b, sems, 12 * k + 10, PT))

    def fourth(k):
        for part in range(2):
            b = line(opp(j), k, part * (side // 2), side // 2)
            remote(b, b, sems, 12 * k + 6 + part, R2).wait_recv()
        b = line(opp(j), k)
        start(remote(b, b, sems, 12 * k + 11, PT))

    def last(k):
        for q, g in enumerate((i, prv(i), nxt(i), opp(i))):
            b = G.at[1 - c, :, g, pl.ds(k * SUB, SUB)]
            remote(b, b, sems, 12 * k + 8 + q, PT).wait_recv()

    chains = []
    for b in range(chunks):
        loads["h%d" % b].wait()
        if b == 0:
            loads["wg"].wait()
            loads["wu"].wait()
        mlp(b)
        chains.append(chain(b))
        next(chains[b])
    loads["wv"].wait()
    for b in range(chunks):
        while True:
            stop = False
            for q in range(b, chunks):
                if next(chains[q], "end") == "end" and q == b:
                    stop = True
            if stop:
                break
        if b == 0:
            logits(0)
    for cp in sent:
        cp.wait_send()
    sent.clear()
    tell(0)
    for b in range(1, chunks):
        logits(b)
        tell(b)
    for b in range(chunks):
        combine(b)
    for k in range(subs + 4):
        for lag, act in ((0, first), (1, second), (2, third), (3, fourth), (4, last)):
            if 0 <= k - lag < subs:
                act(k - lag)
    for b in range(chunks):
        heard(b, lambda cp: cp.wait_send())
    for cp in sent:
        cp.wait_send()


def layout_kernel(side, v_loc, g, st, o, o0, o1, o2):
    r = pl.ds(pl.multiple_of(pl.program_id(0) * o.shape[0], o.shape[0]), o.shape[0])
    for fam in range(2):
        for a in range(side):
            for b in range(side):
                dev = ((b * side + a) * 2) if fam == 0 else ((a * side + b) * 2 + 1)
                o[:, dev * v_loc:(dev + 1) * v_loc] = g[fam, a, b, r, 0:v_loc]
    for q, one in enumerate((o0, o1, o2)):
        one[...] = st[q:q + 1]


def solution(mesh):
    n_dev = mesh.shape["tp"]
    side = math.isqrt(n_dev // 2)

    def device_step(hidden, w_gate, w_up, w_down, norm_gain, w_vocab, temperature, target):
        rows, d = hidden.shape
        f_loc, v_loc = w_gate.shape[1], w_vocab.shape[1]
        vpad = -(-v_loc // 128) * 128
        fpad = -(-f_loc // 128) * 128
        vm = pl.BlockSpec(memory_space=pltpu.VMEM)
        hbm = pl.BlockSpec(memory_space=pl.ANY)
        bf = jnp.bfloat16
        chunks, subs = rows // CHUNK, rows // SUB
        dma = pltpu.SemaphoreType.DMA
        g, stats = pl.pallas_call(
            functools.partial(tail_kernel, side, n_dev, f_loc, v_loc),
            out_shape=(pltpu.VMEM((2, side, side, rows, vpad), bf), pltpu.VMEM((8, rows), jnp.float32)),
            in_specs=[hbm, hbm, hbm, hbm, vm, hbm, vm, vm],
            out_specs=(vm, vm),
            scratch_shapes=[
                pltpu.VMEM((rows, d), bf),
                pltpu.VMEM((2 * fpad, d), bf),
                pltpu.VMEM((fpad, d), bf),
                pltpu.VMEM((rows, d), bf),
                pltpu.VMEM((vpad, d), bf),
                pltpu.VMEM((chunks, vpad, CHUNK), jnp.float32),
                pltpu.VMEM((vpad, 128), jnp.float32),
                pltpu.VMEM((chunks, n_dev, 8, 128), jnp.float32),
                dma((5 + chunks - 1,)),
                dma((24 * chunks,)), dma((24 * chunks,)),
                dma((12 * subs,)), dma((12 * subs,)),
                dma((chunks, n_dev - 1)), dma((chunks, n_dev - 1)),
            ],
            compiler_params=pltpu.CompilerParams(
                collective_id=0, has_side_effects=True, vmem_limit_bytes=30 << 20),
            name="tail",
        )(hidden, w_gate.T, w_up.T, w_down, norm_gain.reshape(1, d), w_vocab.T, temperature.reshape(1, rows),
          target.reshape(1, rows))

        step = 64
        one = jax.ShapeDtypeStruct((1, rows), jnp.float32)
        one_spec = pl.BlockSpec((1, rows), lambda s: (0, 0))
        log_probs, log_norm, entropy, target_logp = pl.pallas_call(
            functools.partial(layout_kernel, side, v_loc),
            out_shape=(jax.ShapeDtypeStruct((rows, n_dev * v_loc), bf), one, one, one),
            grid=(rows // step,),
            in_specs=[vm, vm],
            out_specs=(pl.BlockSpec((step, n_dev * v_loc), lambda s: (s, 0)), one_spec, one_spec, one_spec),
            compiler_params=pltpu.CompilerParams(vmem_limit_bytes=16 << 20),
            name="layout",
        )(g, stats)
        return log_norm.reshape(rows), entropy.reshape(rows), target_logp.reshape(rows), log_probs

    return jax.shard_map(
        device_step,
        mesh=mesh,
        in_specs=(P("dp", None), P(None, "tp"), P(None, "tp"), P("tp", None), P(None),
                  P(None, "tp"), P("dp"), P("dp")),
        out_specs=(P("dp"), P("dp"), P("dp"), P("dp", None)),
        check_vma=False,
    )
```

```python
import functools
import math

import jax
import jax.numpy as jnp
from jax import lax
from jax.experimental import pallas as pl
from jax.experimental.pallas import tpu as pltpu
from jax.sharding import PartitionSpec as P

NORM_EPS = 1e-6
MESH = pl.DeviceIdType.MESH
NT = (((1,), (1,)), ((), ()))
PIECE = 1024
CHUNK = 256
SUB = 128


def place(side):
    me = lax.axis_index("tp")
    c = lax.rem(me, 2)
    chip = lax.div(me, 2)
    x, y = lax.rem(chip, side), lax.div(chip, side)
    i = x * (1 - c) + y * c
    j = y * (1 - c) + x * c
    s1 = 2 + (2 * side - 2) * c
    s2 = 2 * side - (2 * side - 2) * c

    def dev(a, b):
        return a * s1 + b * s2 + c

    nxt = lambda v: lax.rem(v + 1, side)
    prv = lambda v: lax.rem(v + side - 1, side)
    return me, c, i, j, dev(nxt(i), j), dev(prv(i), j), dev(i, nxt(j)), dev(i, prv(j)), me + 1 - 2 * c


def remote(src, dst, sems, k, to):
    return pltpu.make_async_remote_copy(
        src_ref=src, dst_ref=dst, send_sem=sems[0].at[k], recv_sem=sems[1].at[k],
        device_id={"tp": to}, device_id_type=MESH)


def tail_kernel(side, n_dev, f_loc, v_loc, h_hbm, wg_hbm, wu_hbm, wd_hbm, gain, wv_hbm, temp, target, G, out,
                H, W, WD, X, WV, LT, ST, lsem, ssem, rsem, gssem, grsem, stsem, strsem):
    me, c, i, j, R1, L1, R2, L2, PT = place(side)
    rows, d = H.shape
    vpad = WV.shape[0]
    fpad = WD.shape[0]
    pieces = d // PIECE
    half = pieces // 2
    chunks = rows // CHUNK
    subs = rows // SUB
    n1 = CHUNK // 2
    n2 = n1 // side
    f32 = lambda v: v.astype(jnp.float32)
    bf16 = lambda v: v.astype(jnp.bfloat16)
    nxt = lambda v: lax.rem(v + 1, side)
    prv = lambda v: lax.rem(v + side - 1, side)
    opp = lambda v: lax.rem(v + 2, side)

    loads = {}

    def load(name, src, dst):
        cp = pltpu.make_async_copy(src, dst, lsem.at[len(loads)])
        cp.start()
        loads[name] = cp

    load("h0", h_hbm.at[pl.ds(0, CHUNK)], H.at[pl.ds(0, CHUNK)])
    load("wg", wg_hbm, W.at[pl.ds(0, f_loc)])
    load("wu", wu_hbm, W.at[pl.ds(fpad, f_loc)])
    load("wd", wd_hbm, WD.at[pl.ds(0, f_loc)])
    for b in range(1, chunks):
        load("h%d" % b, h_hbm.at[pl.ds(b * CHUNK, CHUNK)], H.at[pl.ds(b * CHUNK, CHUNK)])
    load("wv", wv_hbm, WV.at[pl.ds(0, v_loc)])

    barrier = pltpu.get_barrier_semaphore()

    def greet(t, _):
        to = lax.rem(me + 1 + t, n_dev)
        pl.semaphore_signal(barrier, inc=1, device_id={"tp": to}, device_id_type=MESH)
        return 0
    lax.fori_loop(0, n_dev - 1, greet, 0)
    W[f_loc:fpad] = jnp.zeros((fpad - f_loc, d), W.dtype)
    W[fpad + f_loc:] = jnp.zeros((fpad - f_loc, d), W.dtype)
    WD[f_loc:] = jnp.zeros((fpad - f_loc, d), WD.dtype)
    WV[v_loc:] = jnp.zeros((vpad - v_loc, d), WV.dtype)

    sent, scratch_sent = [], []

    def start(cp, scratch=False):
        cp.start()
        (scratch_sent if scratch else sent).append(cp)
        return cp

    Y = G.at[0, 0]

    def mlp(b):
        gu = lax.dot_general(W[...], H[b * CHUNK:(b + 1) * CHUNK], NT, preferred_element_type=jnp.float32)
        g, u = gu[:fpad], gu[fpad:]
        a = bf16((g * lax.logistic(g) * u).T)
        yield
        if b == 0:
            loads["wd"].wait()
            pl.semaphore_wait(barrier, n_dev - 1)
        for p in range(pieces):
            Y[p, b * CHUNK:(b + 1) * CHUNK] = bf16(
                jnp.dot(a, WD[:, p * PIECE:(p + 1) * PIECE], preferred_element_type=jnp.float32))
            theirs = Y.at[p, pl.ds(pl.multiple_of(b * CHUNK + (1 - c) * n1, n1), n1)]
            start(remote(theirs, G.at[0, 1, p, pl.ds(b * n1, n1)], (ssem, rsem), 24 * b + p, PT), True)

    def chain(b):
        sems = (ssem, rsem)
        k0 = 24 * b
        P0 = G.at[0, 1]
        T = G.at[1, b]
        lo, hi, every = pl.ds(0, half), pl.ds(half, half), pl.ds(0, pieces)
        row1 = lambda g: pl.multiple_of(b * CHUNK + c * n1 + g * n2, n2)

        def add_partner(g):
            at = pl.ds(row1(g), n2)
            frm = pl.ds(pl.multiple_of(b * n1 + g * n2, n2), n2)
            for p in range(pieces):
                Y[p, at] = bf16(f32(Y[p, at]) + f32(P0[p, frm]))

        def ring_sum(pos, row, n, R, L, t0, k, prepare):
            ta, tl, tr = pl.ds(t0, n), pl.ds(t0 + n, n), pl.ds(t0 + 2 * n, n)
            prepare(opp(pos))
            far = pl.ds(row(opp(pos)), n)
            m0 = start(remote(Y.at[lo, far], T.at[lo, ta], sems, k, R), True)
            m1 = start(remote(Y.at[hi, far], T.at[hi, ta], sems, k + 1, L), True)
            prepare(nxt(pos))
            prepare(prv(pos))
            right, left = pl.ds(row(nxt(pos)), n), pl.ds(row(prv(pos)), n)
            yield
            m0.wait_recv()
            for p in range(half):
                Y[p, right] = bf16(f32(Y[p, right]) + f32(T[p, ta]))
            m2 = start(remote(Y.at[every, right], T.at[every, tl], sems, k + 2, R), True)
            m1.wait_recv()
            for p in range(half, pieces):
                Y[p, left] = bf16(f32(Y[p, left]) + f32(T[p, ta]))
            m3 = start(remote(Y.at[every, left], T.at[every, tr], sems, k + 3, L), True)
            prepare(pos)
            yield
            m2.wait_recv()
            m3.wait_recv()
            own = pl.ds(row(pos), n)
            for p in range(pieces):
                total = f32(Y[p, own]) + f32(T[p, tl]) + f32(T[p, tr])
                yield p, total

        def drive(steps, keep):
            for got in steps:
                if got is None:
                    yield
                else:
                    keep(*got)

        yield
        for p in range(pieces):
            box = G.at[0, 1, p, pl.ds(b * n1, n1)]
            remote(box, box, sems, k0 + p, PT).wait_recv()
        own1 = pl.ds(row1(i), n2)
        slot = lambda q: pl.ds(pl.multiple_of(side * n2 + q * n2, n2), n2)

        def keep1(p, total):
            T[p, slot(j)] = bf16(total)
        yield from drive(ring_sum(i, row1, n2, R1, L1, 0, k0 + 4, add_partner), keep1)

        mine, ahead, behind, across = (T.at[:, slot(q)] for q in (j, nxt(j), prv(j), opp(j)))
        start(remote(mine, mine, sems, k0 + 8, R2), True)
        start(remote(mine, mine, sems, k0 + 9, L2), True)
        yield
        remote(behind, behind, sems, k0 + 8, R2).wait_recv()
        part = T.at[lo, slot(prv(j))]
        start(remote(part, part, sems, k0 + 10, R2), True)
        remote(ahead, ahead, sems, k0 + 9, L2).wait_recv()
        part = T.at[hi, slot(nxt(j))]
        start(remote(part, part, sems, k0 + 11, L2), True)
        yield
        for q, ps in ((10, lo), (11, hi)):
            part = T.at[ps, slot(opp(j))]
            remote(part, part, sems, k0 + q, R2).wait_recv()
        sums = []
        square = jnp.zeros((n2, 1), jnp.float32)
        for p in range(pieces):
            y = f32(T[p, slot(0)])
            for q in range(1, side):
                y += f32(T[p, slot(q)])
            r = f32(H[own1, p * PIECE:(p + 1) * PIECE]) + y
            sums.append(r)
            square += jnp.sum(r * r, axis=-1, keepdims=True)
        inv = lax.rsqrt(square / d + NORM_EPS)
        for p in range(pieces):
            cols = slice(p * PIECE, (p + 1) * PIECE)
            X[own1, cols] = bf16(gain[0:1, cols] * sums[p] * inv)
        passed.add(b)

        left_half, right_half = pl.ds(0, d // 2), pl.ds(d // 2, d // 2)

        def ring_gather(pos, row, n, R, L, k):
            at = lambda r, cols=pl.ds(0, d): X.at[pl.ds(r, n), cols]
            own, left, right, far = row(pos), row(prv(pos)), row(nxt(pos)), row(opp(pos))
            start(remote(at(own), at(own), sems, k, R))
            start(remote(at(own), at(own), sems, k + 1, L))
            yield own
            yield
            remote(at(left), at(left), sems, k, R).wait_recv()
            start(remote(at(left, left_half), at(left, left_half), sems, k + 2, R))
            remote(at(right), at(right), sems, k + 1, L).wait_recv()
            start(remote(at(right, right_half), at(right, right_half), sems, k + 3, L))
            yield left
            yield right
            yield
            remote(at(far, left_half), at(far, left_half), sems, k + 2, R).wait_recv()
            remote(at(far, right_half), at(far, right_half), sems, k + 3, L).wait_recv()
            yield far

        k = k0 + 20
        for got in ring_gather(i, row1, n2, R1, L1, k0 + 16):
            if got is None:
                yield
            else:
                line = X.at[pl.ds(got, n2)]
                start(remote(line, line, sems, k, PT))
                k += 1
        yield
        for q, g in enumerate((j, prv(j), nxt(j), opp(j))):
            line = X.at[pl.ds(pl.multiple_of(b * CHUNK + (1 - c) * n1 + g * n2, n2), n2)]
            remote(line, line, sems, k0 + 20 + q, PT).wait_recv()

    vid = lax.broadcasted_iota(jnp.int32, (vpad, CHUNK), 0)

    def logits(b):
        cols = slice(b * CHUNK, (b + 1) * CHUNK)
        l = lax.dot_general(WV[...], X[cols], NT, preferred_element_type=jnp.float32) / temp[0:1, cols]
        LT[b] = l
        real = vid < v_loc
        m = jnp.max(jnp.where(real, l, -jnp.inf), axis=0, keepdims=True)
        e = jnp.where(real, jnp.exp(l - m), 0.0)
        s = jnp.sum(e, axis=0, keepdims=True)
        w = jnp.sum(e * l, axis=0, keepdims=True)
        ids = target[0:1, cols] - me * v_loc
        t = jnp.sum(jnp.where((vid == ids) & real, l, 0.0), axis=0, keepdims=True)
        both = [v[:, h * 128:(h + 1) * 128] for h in range(CHUNK // 128) for v in (m, s, w, t)]
        ST[b, me] = jnp.concatenate(both, axis=0)

    def tell(b):
        def body(t, _):
            to = lax.rem(me + 1 + t, n_dev)
            pltpu.make_async_remote_copy(
                src_ref=ST.at[b, me], dst_ref=ST.at[b, me], send_sem=stsem.at[b, t], recv_sem=strsem.at[b, t],
                device_id={"tp": to}, device_id_type=MESH).start()
            return 0
        lax.fori_loop(0, n_dev - 1, body, 0)

    def heard(b, wait):
        def body(t, _):
            frm = lax.rem(me + n_dev - 1 - t, n_dev)
            cp = pltpu.make_async_remote_copy(
                src_ref=ST.at[b, me], dst_ref=ST.at[b, frm], send_sem=stsem.at[b, t], recv_sem=strsem.at[b, t],
                device_id={"tp": frm}, device_id_type=MESH)
            wait(cp)
            return 0
        lax.fori_loop(0, n_dev - 1, body, 0)

    sems = (gssem, grsem)

    def blk(a, b, k, part=None):
        if part is None:
            return G.at[c, a, b, pl.ds(k * SUB, SUB)]
        return G.at[c, a, b, pl.ds(k * SUB + part * (SUB // 2), SUB // 2)]

    def line(b, k, a0=0, na=side):
        return G.at[c, pl.ds(a0, na), b, pl.ds(k * SUB, SUB)]

    def combine(b):
        heard(b, lambda cp: cp.wait_recv())
        st = ST[b]
        for h in range(CHUNK // 128):
            ms, ss, ws, ts = (st[:, 4 * h + q:4 * h + q + 1, :] for q in range(4))
            m = jnp.max(ms, axis=0)
            f = jnp.exp(ms - m[None])
            s = jnp.sum(ss * f, axis=0)
            w = jnp.sum(ws * f, axis=0)
            t = jnp.sum(ts, axis=0)
            ln = m + jnp.log(s)
            cols = pl.ds(b * CHUNK + h * 128, 128)
            out[0:1, cols] = ln
            out[1:2, cols] = ln - w / s
            out[2:3, cols] = t - ln

            def turn(q, _, h=h, ln=ln):
                v = pl.ds(pl.multiple_of(q * 128, 128), 128)
                G[c, i, j, pl.ds(b * CHUNK + h * 128, 128), v] = bf16((LT[b, v, h * 128:(h + 1) * 128] - ln).T)
                return 0
            lax.fori_loop(0, vpad // 128, turn, 0)
            for k in range((b * CHUNK + h * 128) // SUB, (b * CHUNK + (h + 1) * 128) // SUB):
                own = blk(i, j, k)
                start(remote(own, own, sems, 12 * k, R1))
                start(remote(own, own, sems, 12 * k + 1, L1))

    def first(k):
        left, right = prv(i), nxt(i)
        remote(blk(left, j, k), blk(left, j, k), sems, 12 * k, R1).wait_recv()
        b = blk(left, j, k, 0)
        start(remote(b, b, sems, 12 * k + 2, R1))
        remote(blk(right, j, k), blk(right, j, k), sems, 12 * k + 1, L1).wait_recv()
        b = blk(right, j, k, 1)
        start(remote(b, b, sems, 12 * k + 3, L1))

    def second(k):
        for part in range(2):
            b = blk(opp(i), j, k, part)
            remote(b, b, sems, 12 * k + 2 + part, R1).wait_recv()
        b = line(j, k)
        start(remote(b, b, sems, 12 * k + 4, R2))
        start(remote(b, b, sems, 12 * k + 5, L2))
        start(remote(b, b, sems, 12 * k + 8, PT))

    def third(k):
        b = line(prv(j), k)
        remote(b, b, sems, 12 * k + 4, R2).wait_recv()
        b2 = line(prv(j), k, 0, side // 2)
        start(remote(b2, b2, sems, 12 * k + 6, R2))
        start(remote(b, b, sems, 12 * k + 9, PT))
        b = line(nxt(j), k)
        remote(b, b, sems, 12 * k + 5, L2).wait_recv()
        b2 = line(nxt(j), k, side // 2, side // 2)
        start(remote(b2, b2, sems, 12 * k + 7, L2))
        start(remote(b, b, sems, 12 * k + 10, PT))

    def fourth(k):
        for part in range(2):
            b = line(opp(j), k, part * (side // 2), side // 2)
            remote(b, b, sems, 12 * k + 6 + part, R2).wait_recv()
        b = line(opp(j), k)
        start(remote(b, b, sems, 12 * k + 11, PT))

    def last(k):
        for q, g in enumerate((i, prv(i), nxt(i), opp(i))):
            b = G.at[1 - c, :, g, pl.ds(k * SUB, SUB)]
            remote(b, b, sems, 12 * k + 8 + q, PT).wait_recv()

    passed = set()
    loads["h0"].wait()
    loads["wg"].wait()
    loads["wu"].wait()
    for _ in mlp(0):
        pass
    chains = [chain(b) for b in range(chunks)]
    next(chains[0])
    next(chains[0])
    for b in range(1, chunks):
        loads["h%d" % b].wait()
        for _ in mlp(b):
            next(chains[0])
        next(chains[b])
    loads["wv"].wait()
    while next(chains[0], "end") != "end":
        for b in range(1, chunks):
            next(chains[b], None)
    logits(0)
    assert len(passed) == chunks
    for cp in scratch_sent:
        cp.wait_send()
    tell(0)
    for b in range(1, chunks):
        for _ in chains[b]:
            pass
    combine(0)
    for b in range(1, chunks):
        logits(b)
        tell(b)
    per = CHUNK // SUB
    events = [(k + lag, lag, act, k) for k in range(subs)
              for lag, act in ((0, first), (1, second), (2, third), (3, fourth), (4, last))]
    done = 1
    for when, lag, act, k in sorted(events, key=lambda e: (e[0], e[1])):
        if lag == 0 and k == done * per:
            combine(done)
            done += 1
        act(k)
    for b in range(chunks):
        heard(b, lambda cp: cp.wait_send())
    for cp in sent:
        cp.wait_send()


def layout_kernel(side, v_loc, g, o, stage, sem):
    slots, step, _ = stage.shape
    steps = o.shape[0] // step

    def out(s, slot):
        return pltpu.make_async_copy(stage.at[slot], o.at[pl.ds(pl.multiple_of(s * step, step), step)], sem.at[slot])

    def body(s, _):
        slot = lax.rem(s, slots)

        @pl.when(s >= slots)
        def _():
            out(s - slots, slot).wait()
        r = pl.ds(pl.multiple_of(s * step, step), step)
        for fam in range(2):
            for a in range(side):
                for b in range(side):
                    dev = ((b * side + a) * 2) if fam == 0 else ((a * side + b) * 2 + 1)
                    stage[slot, :, dev * v_loc:(dev + 1) * v_loc] = g[fam, a, b, r, 0:v_loc]
        out(s, slot).start()
        return 0
    lax.fori_loop(0, steps, body, 0)
    for s in range(steps - slots, steps):
        out(s, s % slots).wait()


def solution(mesh):
    n_dev = mesh.shape["tp"]
    side = math.isqrt(n_dev // 2)

    def device_step(hidden, w_gate, w_up, w_down, norm_gain, w_vocab, temperature, target):
        rows, d = hidden.shape
        f_loc, v_loc = w_gate.shape[1], w_vocab.shape[1]
        vpad = -(-v_loc // 128) * 128
        fpad = -(-f_loc // 128) * 128
        vm = pl.BlockSpec(memory_space=pltpu.VMEM)
        hbm = pl.BlockSpec(memory_space=pl.ANY)
        bf = jnp.bfloat16
        chunks, subs = rows // CHUNK, rows // SUB
        dma = pltpu.SemaphoreType.DMA
        g, stats = pl.pallas_call(
            functools.partial(tail_kernel, side, n_dev, f_loc, v_loc),
            out_shape=(pltpu.VMEM((2, side, side, rows, vpad), bf), pltpu.VMEM((8, rows), jnp.float32)),
            in_specs=[hbm, hbm, hbm, hbm, vm, hbm, vm, vm],
            out_specs=(vm, vm),
            scratch_shapes=[
                pltpu.VMEM((rows, d), bf),
                pltpu.VMEM((2 * fpad, d), bf),
                pltpu.VMEM((fpad, d), bf),
                pltpu.VMEM((rows, d), bf),
                pltpu.VMEM((vpad, d), bf),
                pltpu.VMEM((chunks, vpad, CHUNK), jnp.float32),
                pltpu.VMEM((chunks, n_dev, 8, 128), jnp.float32),
                dma((5 + chunks - 1,)),
                dma((24 * chunks,)), dma((24 * chunks,)),
                dma((12 * subs,)), dma((12 * subs,)),
                dma((chunks, n_dev - 1)), dma((chunks, n_dev - 1)),
            ],
            compiler_params=pltpu.CompilerParams(
                collective_id=0, has_side_effects=True, vmem_limit_bytes=30 << 20),
            name="tail",
        )(hidden, w_gate.T, w_up.T, w_down, norm_gain.reshape(1, d), w_vocab.T, temperature.reshape(1, rows),
          target.reshape(1, rows))

        log_probs = pl.pallas_call(
            functools.partial(layout_kernel, side, v_loc),
            out_shape=jax.ShapeDtypeStruct((rows, n_dev * v_loc), bf),
            in_specs=[vm],
            out_specs=hbm,
            scratch_shapes=[pltpu.VMEM((4, 16, n_dev * v_loc), bf), dma((4,))],
            compiler_params=pltpu.CompilerParams(vmem_limit_bytes=16 << 20),
            name="layout",
        )(g)
        return stats[0], stats[1], stats[2], log_probs

    return jax.shard_map(
        device_step,
        mesh=mesh,
        in_specs=(P("dp", None), P(None, "tp"), P(None, "tp"), P("tp", None), P(None),
                  P(None, "tp"), P("dp"), P("dp")),
        out_specs=(P("dp"), P("dp"), P("dp"), P("dp", None)),
        check_vma=False,
    )
```

```python
import functools
import math

import jax
import jax.numpy as jnp
from jax import lax
from jax.experimental import pallas as pl
from jax.experimental.pallas import tpu as pltpu
from jax.sharding import PartitionSpec as P

NORM_EPS = 1e-6
MESH = pl.DeviceIdType.MESH
NT = (((1,), (1,)), ((), ()))
PIECE = 1024
CHUNK = 128
GROUP = 256
LAG = 1

def place(side):
    me = lax.axis_index("tp")
    c = lax.rem(me, 2)
    chip = lax.div(me, 2)
    x, y = lax.rem(chip, side), lax.div(chip, side)
    i = x * (1 - c) + y * c
    j = y * (1 - c) + x * c
    s1 = 2 + (2 * side - 2) * c
    s2 = 2 * side - (2 * side - 2) * c

    def dev(a, b):
        return a * s1 + b * s2 + c

    nxt = lambda v: lax.rem(v + 1, side)
    prv = lambda v: lax.rem(v + side - 1, side)
    return me, c, i, j, dev(nxt(i), j), dev(prv(i), j), dev(i, nxt(j)), dev(i, prv(j)), me + 1 - 2 * c


def remote(src, dst, sems, k, to):
    return pltpu.make_async_remote_copy(
        src_ref=src, dst_ref=dst, send_sem=sems[0].at[k], recv_sem=sems[1].at[k],
        device_id={"tp": to}, device_id_type=MESH)


def tail_kernel(side, n_dev, f_loc, v_loc, h_hbm, wg_hbm, wu_hbm, wd_hbm, gain, wv_hbm, temp, target, G, out,
                H, W, WD, X, WV, LT, ST, lsem, ssem, rsem, gssem, grsem, stsem, strsem):
    me, c, i, j, R1, L1, R2, L2, PT = place(side)
    rows, d = H.shape
    vpad = WV.shape[0]
    fpad = WD.shape[0]
    pieces = d // PIECE
    half = pieces // 2
    chunks = rows // CHUNK
    groups = rows // GROUP
    per = GROUP // CHUNK
    n1 = CHUNK // 2
    n2 = n1 // side
    f32 = lambda v: v.astype(jnp.float32)
    bf16 = lambda v: v.astype(jnp.bfloat16)
    nxt = lambda v: lax.rem(v + 1, side)
    prv = lambda v: lax.rem(v + side - 1, side)
    opp = lambda v: lax.rem(v + 2, side)

    loads = {}

    def load(name, src, dst):
        cp = pltpu.make_async_copy(src, dst, lsem.at[len(loads)])
        cp.start()
        loads[name] = cp

    for p in range(pieces):
        cols = pl.ds(p * PIECE, PIECE)
        load(("h", p), h_hbm.at[pl.ds(0, GROUP), cols], H.at[pl.ds(0, GROUP), cols])
        load(("g", p), wg_hbm.at[:, cols], W.at[pl.ds(0, f_loc), cols])
        load(("u", p), wu_hbm.at[:, cols], W.at[pl.ds(fpad, f_loc), cols])

    barrier = pltpu.get_barrier_semaphore()

    def greet(t, _):
        to = lax.rem(me + 1 + t, n_dev)
        pl.semaphore_signal(barrier, inc=1, device_id={"tp": to}, device_id_type=MESH)
        return 0
    lax.fori_loop(0, n_dev - 1, greet, 0)
    W[f_loc:fpad] = jnp.zeros((fpad - f_loc, d), W.dtype)
    W[fpad + f_loc:] = jnp.zeros((fpad - f_loc, d), W.dtype)
    WD[f_loc:] = jnp.zeros((fpad - f_loc, d), WD.dtype)
    WV[v_loc:] = jnp.zeros((vpad - v_loc, d), WV.dtype)

    sent, scratch_sent = [], [[] for _ in range(chunks)]

    def start(cp, scratch=None):
        cp.start()
        (sent if scratch is None else scratch_sent[scratch]).append(cp)
        return cp

    Y = G.at[0, 0]

    def mlp(b):
        cut = slice(b * GROUP, (b + 1) * GROUP)
        if b == 0:
            gu = None
            for p in range(pieces):
                for name in ("h", "g", "u"):
                    loads[name, p].wait()
                if p == pieces - 1:
                    load("wd", wd_hbm, WD.at[pl.ds(0, f_loc)])
                cols = slice(p * PIECE, (p + 1) * PIECE)
                more = lax.dot_general(W[:, cols], H[cut, cols], NT, preferred_element_type=jnp.float32)
                gu = more if gu is None else gu + more
            for q in range(1, rows // GROUP):
                load("h%d" % q, h_hbm.at[pl.ds(q * GROUP, GROUP)], H.at[pl.ds(q * GROUP, GROUP)])
            load("wv", wv_hbm, WV.at[pl.ds(0, v_loc)])
        else:
            loads["h%d" % b].wait()
            gu = lax.dot_general(W[...], H[cut], NT, preferred_element_type=jnp.float32)
        g, u = gu[:fpad], gu[fpad:]
        a = bf16((g * lax.logistic(g) * u).T)
        yield
        if b == 0:
            loads["wd"].wait()
            pl.semaphore_wait(barrier, n_dev - 1)
        for p in range(pieces):
            Y[p, cut] = bf16(
                jnp.dot(a, WD[:, p * PIECE:(p + 1) * PIECE], preferred_element_type=jnp.float32))
            for q in range(b * GROUP // CHUNK, (b + 1) * GROUP // CHUNK):
                theirs = Y.at[p, pl.ds(pl.multiple_of(q * CHUNK + (1 - c) * n1, n1), n1)]
                start(remote(theirs, G.at[0, 1, p, pl.ds(q * CHUNK, n1)], (ssem, rsem), 26 * q + p, PT), q)

    def chain(b):
        sems = (ssem, rsem)
        k0 = 26 * b
        P0 = G.at[0, 1]
        T = G.at[1, 0]
        lo, hi, every = pl.ds(0, half), pl.ds(half, half), pl.ds(0, pieces)
        row1 = lambda g: pl.multiple_of(b * CHUNK + c * n1 + g * n2, n2)

        def add_partner(g):
            at = pl.ds(row1(g), n2)
            frm = pl.ds(pl.multiple_of(b * CHUNK + g * n2, n2), n2)
            for p in range(pieces):
                Y[p, at] = bf16(f32(Y[p, at]) + f32(P0[p, frm]))

        def ring_sum(pos, row, n, R, L, t0, k, prepare):
            ta, tl, tr = pl.ds(t0, n), pl.ds(t0 + n, n), pl.ds(t0 + 2 * n, n)
            prepare(opp(pos))
            far = pl.ds(row(opp(pos)), n)
            right, left = pl.ds(row(nxt(pos)), n), pl.ds(row(prv(pos)), n)
            m0 = start(remote(Y.at[lo, far], T.at[lo, ta], sems, k, R), b)
            m1 = start(remote(Y.at[hi, far], T.at[hi, ta], sems, k + 1, L), b)
            prepare(nxt(pos))
            m2 = start(remote(Y.at[hi, right], T.at[hi, tl], sems, k + 2, R), b)
            prepare(prv(pos))
            m3 = start(remote(Y.at[lo, left], T.at[lo, tr], sems, k + 3, L), b)
            yield
            m0.wait_recv()
            for p in range(half):
                Y[p, right] = bf16(f32(Y[p, right]) + f32(T[p, ta]))
            m4 = start(remote(Y.at[lo, right], T.at[lo, tl], sems, k + 4, R), b)
            m1.wait_recv()
            for p in range(half, pieces):
                Y[p, left] = bf16(f32(Y[p, left]) + f32(T[p, ta]))
            m5 = start(remote(Y.at[hi, left], T.at[hi, tr], sems, k + 5, L), b)
            prepare(pos)
            yield
            for m in (m2, m3, m4, m5):
                m.wait_recv()
            own = pl.ds(row(pos), n)
            for p in range(pieces):
                total = f32(Y[p, own]) + f32(T[p, tl]) + f32(T[p, tr])
                yield p, total

        def drive(steps, keep):
            for got in steps:
                if got is None:
                    yield
                else:
                    keep(*got)

        yield
        for p in range(pieces):
            box = G.at[0, 1, p, pl.ds(b * CHUNK, n1)]
            remote(box, box, sems, k0 + p, PT).wait_recv()
        own1 = pl.ds(row1(i), n2)
        slot = lambda q: pl.ds(pl.multiple_of(b * CHUNK + side * n2 + q * n2, n2), n2)

        def keep1(p, total):
            T[p, slot(j)] = bf16(total)
        yield from drive(ring_sum(i, row1, n2, R1, L1, b * CHUNK, k0 + 4, add_partner), keep1)

        at = lambda ps, q: T.at[ps, slot(q)]
        for q, (ps, to) in enumerate(((lo, R2), (hi, L2), (hi, R2), (lo, L2))):
            start(remote(at(ps, j), at(ps, j), sems, k0 + 10 + q, to), b)
        yield
        remote(at(lo, prv(j)), at(lo, prv(j)), sems, k0 + 10, R2).wait_recv()
        start(remote(at(lo, prv(j)), at(lo, prv(j)), sems, k0 + 14, R2), b)
        remote(at(hi, nxt(j)), at(hi, nxt(j)), sems, k0 + 11, L2).wait_recv()
        start(remote(at(hi, nxt(j)), at(hi, nxt(j)), sems, k0 + 15, L2), b)
        yield
        for q, ps, frm in ((12, hi, prv(j)), (13, lo, nxt(j)), (14, lo, opp(j)), (15, hi, opp(j))):
            remote(at(ps, frm), at(ps, frm), sems, k0 + q, R2).wait_recv()
        sums = []
        square = jnp.zeros((n2, 1), jnp.float32)
        for p in range(pieces):
            y = f32(T[p, slot(0)])
            for q in range(1, side):
                y += f32(T[p, slot(q)])
            r = f32(H[own1, p * PIECE:(p + 1) * PIECE]) + y
            sums.append(r)
            square += jnp.sum(r * r, axis=-1, keepdims=True)
        inv = lax.rsqrt(square / d + NORM_EPS)
        for p in range(pieces):
            cols = slice(p * PIECE, (p + 1) * PIECE)
            X[own1, cols] = bf16(gain[0:1, cols] * sums[p] * inv)

        left_half, right_half = pl.ds(0, d // 2), pl.ds(d // 2, d // 2)

        at = lambda g, cols=pl.ds(0, d): X.at[pl.ds(row1(g), n2), cols]
        for q, (cols, to) in enumerate(((left_half, R1), (right_half, L1), (right_half, R1), (left_half, L1))):
            start(remote(at(i, cols), at(i, cols), sems, k0 + 16 + q, to))
        start(remote(at(i), at(i), sems, k0 + 22, PT))
        yield
        left, right, far = prv(i), nxt(i), opp(i)
        remote(at(left, left_half), at(left, left_half), sems, k0 + 16, R1).wait_recv()
        start(remote(at(left, left_half), at(left, left_half), sems, k0 + 20, R1))
        remote(at(right, right_half), at(right, right_half), sems, k0 + 17, L1).wait_recv()
        start(remote(at(right, right_half), at(right, right_half), sems, k0 + 21, L1))
        remote(at(left, right_half), at(left, right_half), sems, k0 + 18, R1).wait_recv()
        start(remote(at(left), at(left), sems, k0 + 23, PT))
        remote(at(right, left_half), at(right, left_half), sems, k0 + 19, L1).wait_recv()
        start(remote(at(right), at(right), sems, k0 + 24, PT))
        yield
        remote(at(far, left_half), at(far, left_half), sems, k0 + 20, R1).wait_recv()
        remote(at(far, right_half), at(far, right_half), sems, k0 + 21, L1).wait_recv()
        start(remote(at(far), at(far), sems, k0 + 25, PT))
        yield
        for q, g in enumerate((j, prv(j), nxt(j), opp(j))):
            line = X.at[pl.ds(pl.multiple_of(b * CHUNK + (1 - c) * n1 + g * n2, n2), n2)]
            remote(line, line, sems, k0 + 22 + q, PT).wait_recv()

    vid = lax.broadcasted_iota(jnp.int32, (vpad, GROUP), 0)

    def logits(b):
        cols = slice(b * GROUP, (b + 1) * GROUP)
        l = lax.dot_general(WV[...], X[cols], NT, preferred_element_type=jnp.float32) / temp[0:1, cols]
        LT[b] = l
        real = vid < v_loc
        m = jnp.max(jnp.where(real, l, -jnp.inf), axis=0, keepdims=True)
        e = jnp.where(real, jnp.exp(l - m), 0.0)
        s = jnp.sum(e, axis=0, keepdims=True)
        w = jnp.sum(e * l, axis=0, keepdims=True)
        ids = target[0:1, cols] - me * v_loc
        t = jnp.sum(jnp.where((vid == ids) & real, l, 0.0), axis=0, keepdims=True)
        both = [v[:, h * CHUNK:(h + 1) * CHUNK] for h in range(per) for v in (m, s, w, t)]
        ST[b, me] = jnp.concatenate(both, axis=0)
        for q in range(b * per, (b + 1) * per):
            for cp in scratch_sent[q]:
                cp.wait_send()
        tell(b)

    def tell(b):
        def body(t, _):
            to = lax.rem(me + 1 + t, n_dev)
            pltpu.make_async_remote_copy(
                src_ref=ST.at[b, me], dst_ref=ST.at[b, me], send_sem=stsem.at[b, t], recv_sem=strsem.at[b, t],
                device_id={"tp": to}, device_id_type=MESH).start()
            return 0
        lax.fori_loop(0, n_dev - 1, body, 0)

    def heard(b, wait):
        def body(t, _):
            frm = lax.rem(me + n_dev - 1 - t, n_dev)
            cp = pltpu.make_async_remote_copy(
                src_ref=ST.at[b, me], dst_ref=ST.at[b, frm], send_sem=stsem.at[b, t], recv_sem=strsem.at[b, t],
                device_id={"tp": frm}, device_id_type=MESH)
            wait(cp)
            return 0
        lax.fori_loop(0, n_dev - 1, body, 0)

    sems = (gssem, grsem)

    def blk(a, k, part):
        return G.at[c, a, j, pl.ds(k * CHUNK + part * (CHUNK // 2), CHUNK // 2)]

    def line(b, k):
        return G.at[c, :, b, pl.ds(k * CHUNK, CHUNK)]

    def one_of(a, b, k):
        return G.at[c, a, b, pl.ds(k * CHUNK, CHUNK)]

    def move(ref, k, q, to):
        start(remote(ref, ref, sems, 22 * k + q, to))

    def got(ref, k, q):
        remote(ref, ref, sems, 22 * k + q, PT).wait_recv()

    def combine(b):
        group, part = b // per, b % per
        if part == 0:
            heard(group, lambda cp: cp.wait_recv())
        st = ST[group]
        ms, ss, ws, ts = (st[:, q:q + 1, :] for q in range(4 * part, 4 * part + 4))
        m = jnp.max(ms, axis=0)
        f = jnp.exp(ms - m[None])
        s = jnp.sum(ss * f, axis=0)
        w = jnp.sum(ws * f, axis=0)
        t = jnp.sum(ts, axis=0)
        ln = m + jnp.log(s)
        cols = pl.ds(b * CHUNK, CHUNK)
        out[0:1, cols] = ln
        out[1:2, cols] = ln - w / s
        out[2:3, cols] = t - ln

        def turn(q, _):
            v = pl.ds(pl.multiple_of(q * 128, 128), 128)
            G[c, i, j, cols, v] = bf16((LT[group, v, part * CHUNK:(part + 1) * CHUNK] - ln).T)
            return 0
        lax.fori_loop(0, vpad // 128, turn, 0)
        for q, (bit, to) in enumerate(((0, R1), (1, L1), (1, R1), (0, L1))):
            move(blk(i, b, bit), b, q, to)

    def first(k):
        left, right = prv(i), nxt(i)
        got(blk(left, k, 0), k, 0)
        move(blk(left, k, 0), k, 4, R1)
        got(blk(right, k, 1), k, 1)
        move(blk(right, k, 1), k, 5, L1)

    def second(k):
        got(blk(prv(i), k, 1), k, 2)
        got(blk(nxt(i), k, 0), k, 3)
        got(blk(opp(i), k, 0), k, 4)
        got(blk(opp(i), k, 1), k, 5)
        move(line(j, k), k, 18, PT)

    toR = tuple(range(side))
    toL = toR[side // 2:] + toR[:side // 2]

    def send(k, q):
        move(one_of(toR[q], j, k), k, 6 + q, R2)
        move(one_of(toL[q], j, k), k, 6 + side + q, L2)

    def third(k):
        for q in range(side // 2):
            b = one_of(toR[q], prv(j), k)
            got(b, k, 6 + q)
            move(b, k, 6 + 2 * side + q, R2)
            b = one_of(toL[q], nxt(j), k)
            got(b, k, 6 + side + q)
            move(b, k, 6 + 2 * side + side // 2 + q, L2)

    def fourth(k):
        for q in range(side // 2, side):
            got(one_of(toR[q], prv(j), k), k, 6 + q)
        move(line(prv(j), k), k, 19, PT)
        for q in range(side // 2, side):
            got(one_of(toL[q], nxt(j), k), k, 6 + side + q)
        move(line(nxt(j), k), k, 20, PT)
        for q in range(side // 2):
            got(one_of(toR[q], opp(j), k), k, 6 + 2 * side + q)
            got(one_of(toL[q], opp(j), k), k, 6 + 2 * side + side // 2 + q)
        move(line(opp(j), k), k, 21, PT)

    def last(k):
        for q, g in enumerate((i, prv(i), nxt(i), opp(i))):
            got(G.at[1 - c, :, g, pl.ds(k * CHUNK, CHUNK)], k, 18 + q)

    def lockstep(g):
        mine = [chain(b) for b in range(g * per, (g + 1) * per)]
        for one in mine:
            next(one)
        ended = False
        while not ended:
            for one in mine:
                ended = next(one, "end") == "end"
            if not ended:
                yield

    assert groups == 2 and per == 2
    for _ in mlp(0):
        pass
    one, two = lockstep(0), lockstep(1)
    next(one)
    for _ in mlp(1):
        next(one)
    loads["wv"].wait()
    rnd = 0
    while next(one, "end") != "end":
        rnd += 1
        if rnd > LAG:
            next(two)
    def both(k):
        second(k)
        for q in range(side):
            send(k, q)

    logits(0)
    next(two)
    combine(0)
    combine(1)
    next(two, None)
    first(0)
    next(two, None)
    second(0)
    send(0, 0)
    first(1)
    next(two, None)
    send(0, 1)
    for _ in two:
        pass
    send(0, 2)
    logits(1)
    send(0, 3)
    third(0)
    both(1)
    combine(2)
    combine(3)
    for act, k in ((first, 2), (third, 1), (first, 3), (fourth, 0), (both, 2), (fourth, 1), (both, 3), (last, 0),
                   (third, 2), (last, 1), (third, 3), (fourth, 2), (last, 2), (fourth, 3), (last, 3)):
        act(k)
    for b in range(groups):
        heard(b, lambda cp: cp.wait_send())
    for cp in sent:
        cp.wait_send()


def layout_kernel(side, v_loc, g, o, stage, sem):
    slots, step, _ = stage.shape
    steps = o.shape[0] // step

    def out(s, slot):
        return pltpu.make_async_copy(stage.at[slot], o.at[pl.ds(pl.multiple_of(s * step, step), step)], sem.at[slot])

    def body(s, _):
        slot = lax.rem(s, slots)

        @pl.when(s >= slots)
        def _():
            out(s - slots, slot).wait()
        r = pl.ds(pl.multiple_of(s * step, step), step)
        for fam in range(2):
            for a in range(side):
                for b in range(side):
                    dev = ((b * side + a) * 2) if fam == 0 else ((a * side + b) * 2 + 1)
                    stage[slot, :, dev * v_loc:(dev + 1) * v_loc] = g[fam, a, b, r, 0:v_loc]
        out(s, slot).start()
        return 0
    lax.fori_loop(0, steps, body, 0)
    for s in range(steps - slots, steps):
        out(s, s % slots).wait()


def solution(mesh):
    n_dev = mesh.shape["tp"]
    side = math.isqrt(n_dev // 2)

    def device_step(hidden, w_gate, w_up, w_down, norm_gain, w_vocab, temperature, target):
        rows, d = hidden.shape
        f_loc, v_loc = w_gate.shape[1], w_vocab.shape[1]
        vpad = -(-v_loc // 128) * 128
        fpad = -(-f_loc // 128) * 128
        vm = pl.BlockSpec(memory_space=pltpu.VMEM)
        hbm = pl.BlockSpec(memory_space=pl.ANY)
        bf = jnp.bfloat16
        chunks, groups = rows // CHUNK, rows // GROUP
        dma = pltpu.SemaphoreType.DMA
        g, stats = pl.pallas_call(
            functools.partial(tail_kernel, side, n_dev, f_loc, v_loc),
            out_shape=(pltpu.VMEM((2, side, side, rows, vpad), bf), pltpu.VMEM((8, rows), jnp.float32)),
            in_specs=[hbm, hbm, hbm, hbm, vm, hbm, vm, vm],
            out_specs=(vm, vm),
            scratch_shapes=[
                pltpu.VMEM((rows, d), bf),
                pltpu.VMEM((2 * fpad, d), bf),
                pltpu.VMEM((fpad, d), bf),
                pltpu.VMEM((rows, d), bf),
                pltpu.VMEM((vpad, d), bf),
                pltpu.VMEM((groups, vpad, GROUP), jnp.float32),
                pltpu.VMEM((groups, n_dev, 8, CHUNK), jnp.float32),
                dma((3 * (d // PIECE) + groups + 1,)),
                dma((26 * chunks,)), dma((26 * chunks,)),
                dma((22 * chunks,)), dma((22 * chunks,)),
                dma((groups, n_dev - 1)), dma((groups, n_dev - 1)),
            ],
            compiler_params=pltpu.CompilerParams(
                collective_id=0, has_side_effects=True, vmem_limit_bytes=30 << 20),
            name="tail",
        )(hidden, w_gate.T, w_up.T, w_down, norm_gain.reshape(1, d), w_vocab.T, temperature.reshape(1, rows),
          target.reshape(1, rows))

        log_probs = pl.pallas_call(
            functools.partial(layout_kernel, side, v_loc),
            out_shape=jax.ShapeDtypeStruct((rows, n_dev * v_loc), bf),
            in_specs=[vm],
            out_specs=hbm,
            scratch_shapes=[pltpu.VMEM((4, 16, n_dev * v_loc), bf), dma((4,))],
            compiler_params=pltpu.CompilerParams(vmem_limit_bytes=16 << 20),
            name="layout",
        )(g)
        return stats[0], stats[1], stats[2], log_probs

    return jax.shard_map(
        device_step,
        mesh=mesh,
        in_specs=(P("dp", None), P(None, "tp"), P(None, "tp"), P("tp", None), P(None),
                  P(None, "tp"), P("dp"), P("dp")),
        out_specs=(P("dp"), P("dp"), P("dp"), P("dp", None)),
        check_vma=False,
    )
```

```python
import functools
import math

import jax
import jax.numpy as jnp
from jax import lax
from jax.experimental import pallas as pl
from jax.experimental.pallas import tpu as pltpu
from jax.sharding import PartitionSpec as P

NORM_EPS = 1e-6
MESH = pl.DeviceIdType.MESH
NT = (((1,), (1,)), ((), ()))
PIECE = 1024
CHUNK = 128
GROUP = 256
BEFORE = 2
SETTLE = 4
LAG = 1

def place(side):
    me = lax.axis_index("tp")
    c = lax.rem(me, 2)
    chip = lax.div(me, 2)
    x, y = lax.rem(chip, side), lax.div(chip, side)
    i = x * (1 - c) + y * c
    j = y * (1 - c) + x * c
    s1 = 2 + (2 * side - 2) * c
    s2 = 2 * side - (2 * side - 2) * c

    def dev(a, b):
        return a * s1 + b * s2 + c

    nxt = lambda v: lax.rem(v + 1, side)
    prv = lambda v: lax.rem(v + side - 1, side)
    return me, c, i, j, dev(nxt(i), j), dev(prv(i), j), dev(i, nxt(j)), dev(i, prv(j)), me + 1 - 2 * c


def remote(src, dst, sems, k, to):
    return pltpu.make_async_remote_copy(
        src_ref=src, dst_ref=dst, send_sem=sems[0].at[k], recv_sem=sems[1].at[k],
        device_id={"tp": to}, device_id_type=MESH)


def tail_kernel(side, n_dev, f_loc, v_loc, h_hbm, wg_hbm, wu_hbm, wd_hbm, gain, wv_hbm, temp, target, G, out,
                H, W, WD, X, WV, LT, ST, lsem, ssem, rsem, gssem, grsem, stsem, strsem):
    me, c, i, j, R1, L1, R2, L2, PT = place(side)
    rows, d = H.shape
    vpad = WV.shape[0]
    fpad = WD.shape[0]
    pieces = d // PIECE
    half = pieces // 2
    chunks = rows // CHUNK
    groups = rows // GROUP
    per = GROUP // CHUNK
    n1 = CHUNK // 2
    n2 = n1 // side
    f32 = lambda v: v.astype(jnp.float32)
    bf16 = lambda v: v.astype(jnp.bfloat16)
    nxt = lambda v: lax.rem(v + 1, side)
    prv = lambda v: lax.rem(v + side - 1, side)
    opp = lambda v: lax.rem(v + 2, side)

    loads = {}

    def load(name, src, dst):
        cp = pltpu.make_async_copy(src, dst, lsem.at[len(loads)])
        cp.start()
        loads[name] = cp

    for p in range(pieces):
        cols = pl.ds(p * PIECE, PIECE)
        load(("h", p), h_hbm.at[pl.ds(0, GROUP), cols], H.at[pl.ds(0, GROUP), cols])
        load(("g", p), wg_hbm.at[:, cols], W.at[pl.ds(0, f_loc), cols])
        load(("u", p), wu_hbm.at[:, cols], W.at[pl.ds(fpad, f_loc), cols])

    barrier = pltpu.get_barrier_semaphore()

    def greet(t, _):
        to = lax.rem(me + 1 + t, n_dev)
        pl.semaphore_signal(barrier, inc=1, device_id={"tp": to}, device_id_type=MESH)
        return 0
    lax.fori_loop(0, n_dev - 1, greet, 0)
    W[f_loc:fpad] = jnp.zeros((fpad - f_loc, d), W.dtype)
    W[fpad + f_loc:] = jnp.zeros((fpad - f_loc, d), W.dtype)
    WD[f_loc:] = jnp.zeros((fpad - f_loc, d), WD.dtype)
    WV[v_loc:] = jnp.zeros((vpad - v_loc, d), WV.dtype)

    sent, scratch_sent = [], [[] for _ in range(chunks)]

    def start(cp, scratch=None):
        cp.start()
        (sent if scratch is None else scratch_sent[scratch]).append(cp)
        return cp

    Y = G.at[0, 0]

    def mlp(b):
        cut = slice(b * GROUP, (b + 1) * GROUP)
        if b == 0:
            gu = None
            for p in range(pieces):
                for name in ("h", "g", "u"):
                    loads[name, p].wait()
                if p == pieces - 1:
                    load("wd", wd_hbm, WD.at[pl.ds(0, f_loc)])
                cols = slice(p * PIECE, (p + 1) * PIECE)
                more = lax.dot_general(W[:, cols], H[cut, cols], NT, preferred_element_type=jnp.float32)
                gu = more if gu is None else gu + more
            for q in range(1, rows // GROUP):
                load("h%d" % q, h_hbm.at[pl.ds(q * GROUP, GROUP)], H.at[pl.ds(q * GROUP, GROUP)])
            load("wv", wv_hbm, WV.at[pl.ds(0, v_loc)])
        else:
            loads["h%d" % b].wait()
            gu = lax.dot_general(W[...], H[cut], NT, preferred_element_type=jnp.float32)
        g, u = gu[:fpad], gu[fpad:]
        a = bf16((g * lax.logistic(g) * u).T)
        yield
        if b == 0:
            loads["wd"].wait()
        for p in range(pieces):
            Y[p, cut] = bf16(
                jnp.dot(a, WD[:, p * PIECE:(p + 1) * PIECE], preferred_element_type=jnp.float32))
            if b == 0 and p < BEFORE:
                continue
            if b == 0 and p == BEFORE:
                pl.semaphore_wait(barrier, n_dev - 1)
            for p2 in range(p + 1) if b == 0 and p == BEFORE else (p,):
                for q in range(b * per, (b + 1) * per):
                    theirs = Y.at[p2, pl.ds(pl.multiple_of(q * CHUNK + (1 - c) * n1, n1), n1)]
                    start(remote(theirs, G.at[0, 1, p2, pl.ds(q * CHUNK, n1)], (ssem, rsem), 26 * q + p2, PT), q)

    def chain(b):
        sems = (ssem, rsem)
        k0 = 26 * b
        P0 = G.at[0, 1]
        T = G.at[1, 0]
        lo, hi, every = pl.ds(0, half), pl.ds(half, half), pl.ds(0, pieces)
        row1 = lambda g: pl.multiple_of(b * CHUNK + c * n1 + g * n2, n2)

        def add_partner(g):
            at = pl.ds(row1(g), n2)
            frm = pl.ds(pl.multiple_of(b * CHUNK + g * n2, n2), n2)
            for p in range(pieces):
                Y[p, at] = bf16(f32(Y[p, at]) + f32(P0[p, frm]))

        def ring_sum(pos, row, n, R, L, t0, k, prepare):
            ta, tl, tr = pl.ds(t0, n), pl.ds(t0 + n, n), pl.ds(t0 + 2 * n, n)
            prepare(opp(pos))
            far = pl.ds(row(opp(pos)), n)
            right, left = pl.ds(row(nxt(pos)), n), pl.ds(row(prv(pos)), n)
            m0 = start(remote(Y.at[lo, far], T.at[lo, ta], sems, k, R), b)
            m1 = start(remote(Y.at[hi, far], T.at[hi, ta], sems, k + 1, L), b)
            prepare(nxt(pos))
            m2 = start(remote(Y.at[hi, right], T.at[hi, tl], sems, k + 2, R), b)
            prepare(prv(pos))
            m3 = start(remote(Y.at[lo, left], T.at[lo, tr], sems, k + 3, L), b)
            yield
            m0.wait_recv()
            for p in range(half):
                Y[p, right] = bf16(f32(Y[p, right]) + f32(T[p, ta]))
            m4 = start(remote(Y.at[lo, right], T.at[lo, tl], sems, k + 4, R), b)
            m1.wait_recv()
            for p in range(half, pieces):
                Y[p, left] = bf16(f32(Y[p, left]) + f32(T[p, ta]))
            m5 = start(remote(Y.at[hi, left], T.at[hi, tr], sems, k + 5, L), b)
            prepare(pos)
            yield
            for m in (m2, m3, m4, m5):
                m.wait_recv()
            own = pl.ds(row(pos), n)
            for p in range(pieces):
                total = f32(Y[p, own]) + f32(T[p, tl]) + f32(T[p, tr])
                yield p, total

        def drive(steps, keep):
            for got in steps:
                if got is None:
                    yield
                else:
                    keep(*got)

        yield
        for p in range(pieces):
            box = G.at[0, 1, p, pl.ds(b * CHUNK, n1)]
            remote(box, box, sems, k0 + p, PT).wait_recv()
        own1 = pl.ds(row1(i), n2)
        slot = lambda q: pl.ds(pl.multiple_of(b * CHUNK + side * n2 + q * n2, n2), n2)

        def keep1(p, total):
            T[p, slot(j)] = bf16(total)
        yield from drive(ring_sum(i, row1, n2, R1, L1, b * CHUNK, k0 + 4, add_partner), keep1)

        at = lambda ps, q: T.at[ps, slot(q)]
        for q, (ps, to) in enumerate(((lo, R2), (hi, L2), (hi, R2), (lo, L2))):
            start(remote(at(ps, j), at(ps, j), sems, k0 + 10 + q, to), b)
        yield
        remote(at(lo, prv(j)), at(lo, prv(j)), sems, k0 + 10, R2).wait_recv()
        start(remote(at(lo, prv(j)), at(lo, prv(j)), sems, k0 + 14, R2), b)
        remote(at(hi, nxt(j)), at(hi, nxt(j)), sems, k0 + 11, L2).wait_recv()
        start(remote(at(hi, nxt(j)), at(hi, nxt(j)), sems, k0 + 15, L2), b)
        yield
        for q, ps, frm in ((12, hi, prv(j)), (13, lo, nxt(j)), (14, lo, opp(j)), (15, hi, opp(j))):
            remote(at(ps, frm), at(ps, frm), sems, k0 + q, R2).wait_recv()
        sums = []
        square = jnp.zeros((n2, 1), jnp.float32)
        for p in range(pieces):
            y = f32(T[p, slot(0)])
            for q in range(1, side):
                y += f32(T[p, slot(q)])
            r = f32(H[own1, p * PIECE:(p + 1) * PIECE]) + y
            sums.append(r)
            square += jnp.sum(r * r, axis=-1, keepdims=True)
        inv = lax.rsqrt(square / d + NORM_EPS)
        for p in range(pieces):
            cols = slice(p * PIECE, (p + 1) * PIECE)
            X[own1, cols] = bf16(gain[0:1, cols] * sums[p] * inv)

        left_half, right_half = pl.ds(0, d // 2), pl.ds(d // 2, d // 2)

        at = lambda g, cols=pl.ds(0, d): X.at[pl.ds(row1(g), n2), cols]
        for q, (cols, to) in enumerate(((left_half, R1), (right_half, L1), (right_half, R1), (left_half, L1))):
            start(remote(at(i, cols), at(i, cols), sems, k0 + 16 + q, to))
        start(remote(at(i), at(i), sems, k0 + 22, PT))
        yield
        left, right, far = prv(i), nxt(i), opp(i)
        remote(at(left, left_half), at(left, left_half), sems, k0 + 16, R1).wait_recv()
        start(remote(at(left, left_half), at(left, left_half), sems, k0 + 20, R1))
        remote(at(right, right_half), at(right, right_half), sems, k0 + 17, L1).wait_recv()
        start(remote(at(right, right_half), at(right, right_half), sems, k0 + 21, L1))
        remote(at(left, right_half), at(left, right_half), sems, k0 + 18, R1).wait_recv()
        start(remote(at(left), at(left), sems, k0 + 23, PT))
        remote(at(right, left_half), at(right, left_half), sems, k0 + 19, L1).wait_recv()
        start(remote(at(right), at(right), sems, k0 + 24, PT))
        yield
        remote(at(far, left_half), at(far, left_half), sems, k0 + 20, R1).wait_recv()
        remote(at(far, right_half), at(far, right_half), sems, k0 + 21, L1).wait_recv()
        start(remote(at(far), at(far), sems, k0 + 25, PT))
        yield
        for q, g in enumerate((j, prv(j), nxt(j), opp(j))):
            line = X.at[pl.ds(pl.multiple_of(b * CHUNK + (1 - c) * n1 + g * n2, n2), n2)]
            remote(line, line, sems, k0 + 22 + q, PT).wait_recv()

    vid = lax.broadcasted_iota(jnp.int32, (vpad, GROUP), 0)

    def logits(b):
        cols = slice(b * GROUP, (b + 1) * GROUP)
        l = lax.dot_general(WV[...], X[cols], NT, preferred_element_type=jnp.float32) / temp[0:1, cols]
        LT[b] = l
        real = vid < v_loc
        m = jnp.max(jnp.where(real, l, -jnp.inf), axis=0, keepdims=True)
        e = jnp.where(real, jnp.exp(l - m), 0.0)
        s = jnp.sum(e, axis=0, keepdims=True)
        w = jnp.sum(e * l, axis=0, keepdims=True)
        ids = target[0:1, cols] - me * v_loc
        t = jnp.sum(jnp.where((vid == ids) & real, l, 0.0), axis=0, keepdims=True)
        both = [v[:, h * CHUNK:(h + 1) * CHUNK] for h in range(per) for v in (m, s, w, t)]
        ST[b, me] = jnp.concatenate(both, axis=0)
        for q in range(b * per, (b + 1) * per):
            for cp in scratch_sent[q]:
                cp.wait_send()
        tell(b)

    def tell(b):
        def body(t, _):
            to = lax.rem(me + 1 + t, n_dev)
            pltpu.make_async_remote_copy(
                src_ref=ST.at[b, me], dst_ref=ST.at[b, me], send_sem=stsem.at[b, t], recv_sem=strsem.at[b, t],
                device_id={"tp": to}, device_id_type=MESH).start()
            return 0
        lax.fori_loop(0, n_dev - 1, body, 0, unroll=True)

    def heard(b, wait):
        def body(t, _):
            frm = lax.rem(me + n_dev - 1 - t, n_dev)
            cp = pltpu.make_async_remote_copy(
                src_ref=ST.at[b, me], dst_ref=ST.at[b, frm], send_sem=stsem.at[b, t], recv_sem=strsem.at[b, t],
                device_id={"tp": frm}, device_id_type=MESH)
            wait(cp)
            return 0
        lax.fori_loop(0, n_dev - 1, body, 0, unroll=True)

    sems = (gssem, grsem)

    def blk(a, k, part):
        return G.at[c, a, j, pl.ds(k * CHUNK + part * (CHUNK // 2), CHUNK // 2)]

    def line(b, k):
        return G.at[c, :, b, pl.ds(k * CHUNK, CHUNK)]

    def one_of(a, b, k):
        return G.at[c, a, b, pl.ds(k * CHUNK, CHUNK)]

    def move(ref, k, q, to):
        start(remote(ref, ref, sems, 25 * k + q, to))

    def got(ref, k, q):
        remote(ref, ref, sems, 25 * k + q, PT).wait_recv()

    def combine(b):
        group, part = b // per, b % per
        if part == 0:
            heard(group, lambda cp: cp.wait_recv())
        st = ST[group]
        ms, ss, ws, ts = (st[:, q:q + 1, :] for q in range(4 * part, 4 * part + 4))
        m = jnp.max(ms, axis=0)
        f = jnp.exp(ms - m[None])
        s = jnp.sum(ss * f, axis=0)
        w = jnp.sum(ws * f, axis=0)
        t = jnp.sum(ts, axis=0)
        ln = m + jnp.log(s)
        cols = pl.ds(b * CHUNK, CHUNK)
        out[0:1, cols] = ln
        out[1:2, cols] = ln - w / s
        out[2:3, cols] = t - ln

        def turn(q, _):
            v = pl.ds(pl.multiple_of(q * 128, 128), 128)
            G[c, i, j, cols, v] = bf16((LT[group, v, part * CHUNK:(part + 1) * CHUNK] - ln).T)
            return 0
        lax.fori_loop(0, vpad // 128, turn, 0)
        for q, (bit, to) in enumerate(((0, R1), (1, L1), (1, R1), (0, L1))):
            move(blk(i, b, bit), b, q, to)

    def first(k):
        left, right = prv(i), nxt(i)
        got(blk(left, k, 0), k, 0)
        move(blk(left, k, 0), k, 4, R1)
        got(blk(right, k, 1), k, 1)
        move(blk(right, k, 1), k, 5, L1)

    OWN, LEFT, RIGHT, FAR = range(4)
    stand = (i, prv(i), nxt(i), opp(i))

    def send(k, z, right=True, left=True):
        b = one_of(stand[z], j, k)
        if right:
            move(b, k, 6 + z, R2)
        if left:
            move(b, k, 10 + z, L2)

    def sides(k):
        got(blk(prv(i), k, 1), k, 2)
        got(blk(nxt(i), k, 0), k, 3)

    def far_side(k):
        got(blk(opp(i), k, 0), k, 4)
        got(blk(opp(i), k, 1), k, 5)

    def second(k):
        far_side(k)
        send(k, FAR)
        move(line(j, k), k, 18, PT)

    def third(k):
        for z, base, frm, sem, to in ((OWN, 6, prv(j), 14, R2), (LEFT, 10, nxt(j), 16, L2),
                                      (RIGHT, 6, prv(j), 15, R2), (FAR, 10, nxt(j), 17, L2)):
            b = one_of(stand[z], frm, k)
            got(b, k, base + z)
            move(b, k, sem, to)

    def fourth(k):
        for z in (LEFT, FAR):
            got(one_of(stand[z], prv(j), k), k, 6 + z)
        move(line(prv(j), k), k, 19, PT)
        for z in (OWN, RIGHT):
            got(one_of(stand[z], nxt(j), k), k, 10 + z)
        move(line(nxt(j), k), k, 20, PT)
        for z, sem in ((OWN, 14), (LEFT, 16), (RIGHT, 15), (FAR, 17)):
            b = one_of(stand[z], opp(j), k)
            got(b, k, sem)
            move(b, k, 21 + z, PT)

    def last(k):
        for q, g in enumerate((i, prv(i), nxt(i))):
            got(G.at[1 - c, :, g, pl.ds(k * CHUNK, CHUNK)], k, 18 + q)
        for z, a in enumerate((j, prv(j), nxt(j), opp(j))):
            got(G.at[1 - c, a, opp(i), pl.ds(k * CHUNK, CHUNK)], k, 21 + z)

    def lockstep(g):
        mine = [chain(b) for b in range(g * per, (g + 1) * per)]
        for one in mine:
            next(one)
        ended = False
        while not ended:
            for one in mine:
                ended = next(one, "end") == "end"
            if not ended:
                yield

    assert groups == 2 and per == 2
    for _ in mlp(0):
        pass
    one, two = lockstep(0), lockstep(1)
    next(one)
    for _ in mlp(1):
        next(one)
    loads["wv"].wait()
    rnd = 0
    while next(one, "end") != "end":
        rnd += 1
        if rnd > LAG:
            next(two)
    def both(k):
        sides(k)
        far_side(k)
        for zr, zl in ((OWN, LEFT), (RIGHT, FAR), (LEFT, OWN), (FAR, RIGHT)):
            send(k, zr, left=False)
            send(k, zl, right=False)
        move(line(j, k), k, 18, PT)

    logits(0)
    next(two)
    combine(0)
    send(0, OWN)
    combine(1)
    next(two, None)
    first(0)
    next(two, None)
    sides(0)
    send(0, LEFT)
    next(two, None)
    send(0, RIGHT)
    first(1)
    for _ in two:
        pass
    second(0)
    logits(1)
    third(0)
    both(1)
    combine(2)
    combine(3)
    for b in range(groups):
        heard(b, lambda cp: cp.wait_send())
    marks = [0] * SETTLE
    settled = 0
    for act, k in ((first, 2), (third, 1), (first, 3), (fourth, 0), (both, 2), (fourth, 1), (both, 3), (last, 0),
                   (third, 2), (last, 1), (third, 3), (fourth, 2), (last, 2), (fourth, 3), (last, 3)):
        upto = marks[-SETTLE]
        for cp in sent[settled:upto]:
            cp.wait_send()
        settled = max(settled, upto)
        marks.append(len(sent))
        act(k)
    for cp in sent[settled:]:
        cp.wait_send()


def layout_kernel(side, v_loc, g, o, stage, sem):
    slots, step, _ = stage.shape
    steps = o.shape[0] // step

    def out(s, slot):
        return pltpu.make_async_copy(stage.at[slot], o.at[pl.ds(pl.multiple_of(s * step, step), step)], sem.at[slot])

    def body(s, _):
        slot = lax.rem(s, slots)

        @pl.when(s >= slots)
        def _():
            out(s - slots, slot).wait()
        r = pl.ds(pl.multiple_of(s * step, step), step)
        for fam in range(2):
            for a in range(side):
                for b in range(side):
                    dev = ((b * side + a) * 2) if fam == 0 else ((a * side + b) * 2 + 1)
                    stage[slot, :, dev * v_loc:(dev + 1) * v_loc] = g[fam, a, b, r, 0:v_loc]
        out(s, slot).start()
        return 0
    lax.fori_loop(0, steps, body, 0)
    for s in range(steps - slots, steps):
        out(s, s % slots).wait()


def solution(mesh):
    n_dev = mesh.shape["tp"]
    side = math.isqrt(n_dev // 2)

    def device_step(hidden, w_gate, w_up, w_down, norm_gain, w_vocab, temperature, target):
        rows, d = hidden.shape
        f_loc, v_loc = w_gate.shape[1], w_vocab.shape[1]
        vpad = -(-v_loc // 128) * 128
        fpad = -(-f_loc // 128) * 128
        vm = pl.BlockSpec(memory_space=pltpu.VMEM)
        hbm = pl.BlockSpec(memory_space=pl.ANY)
        bf = jnp.bfloat16
        chunks, groups = rows // CHUNK, rows // GROUP
        dma = pltpu.SemaphoreType.DMA
        g, stats = pl.pallas_call(
            functools.partial(tail_kernel, side, n_dev, f_loc, v_loc),
            out_shape=(pltpu.VMEM((2, side, side, rows, vpad), bf), pltpu.VMEM((8, rows), jnp.float32)),
            in_specs=[hbm, hbm, hbm, hbm, vm, hbm, vm, vm],
            out_specs=(vm, vm),
            scratch_shapes=[
                pltpu.VMEM((rows, d), bf),
                pltpu.VMEM((2 * fpad, d), bf),
                pltpu.VMEM((fpad, d), bf),
                pltpu.VMEM((rows, d), bf),
                pltpu.VMEM((vpad, d), bf),
                pltpu.VMEM((groups, vpad, GROUP), jnp.float32),
                pltpu.VMEM((groups, n_dev, 8, CHUNK), jnp.float32),
                dma((3 * (d // PIECE) + groups + 1,)),
                dma((26 * chunks,)), dma((26 * chunks,)),
                dma((25 * chunks,)), dma((25 * chunks,)),
                dma((groups, n_dev - 1)), dma((groups, n_dev - 1)),
            ],
            compiler_params=pltpu.CompilerParams(
                collective_id=0, has_side_effects=True, vmem_limit_bytes=30 << 20),
            name="tail",
        )(hidden, w_gate.T, w_up.T, w_down, norm_gain.reshape(1, d), w_vocab.T, temperature.reshape(1, rows),
          target.reshape(1, rows))

        log_probs = pl.pallas_call(
            functools.partial(layout_kernel, side, v_loc),
            out_shape=jax.ShapeDtypeStruct((rows, n_dev * v_loc), bf),
            in_specs=[vm],
            out_specs=hbm,
            scratch_shapes=[pltpu.VMEM((4, 16, n_dev * v_loc), bf), dma((4,))],
            compiler_params=pltpu.CompilerParams(vmem_limit_bytes=16 << 20),
            name="layout",
        )(g)
        return stats[0], stats[1], stats[2], log_probs

    return jax.shard_map(
        device_step,
        mesh=mesh,
        in_specs=(P("dp", None), P(None, "tp"), P(None, "tp"), P("tp", None), P(None),
                  P(None, "tp"), P("dp"), P("dp")),
        out_specs=(P("dp"), P("dp"), P("dp"), P("dp", None)),
        check_vma=False,
    )
```

```python
import functools
import math

import jax
import jax.numpy as jnp
from jax import lax
from jax.experimental import pallas as pl
from jax.experimental.pallas import tpu as pltpu
from jax.sharding import PartitionSpec as P

NORM_EPS = 1e-6
MESH = pl.DeviceIdType.MESH
NT = (((1,), (1,)), ((), ()))
PIECE = 1024
CHUNK = 128
GROUP = 256
BEFORE = 2
SETTLE = 4
LAG = 1

def place(side):
    me = lax.axis_index("tp")
    c = lax.rem(me, 2)
    chip = lax.div(me, 2)
    x, y = lax.rem(chip, side), lax.div(chip, side)
    i = x * (1 - c) + y * c
    j = y * (1 - c) + x * c
    s1 = 2 + (2 * side - 2) * c
    s2 = 2 * side - (2 * side - 2) * c

    def dev(a, b):
        return a * s1 + b * s2 + c

    nxt = lambda v: lax.rem(v + 1, side)
    prv = lambda v: lax.rem(v + side - 1, side)
    return me, c, i, j, dev(nxt(i), j), dev(prv(i), j), dev(i, nxt(j)), dev(i, prv(j)), me + 1 - 2 * c


def remote(src, dst, sems, k, to):
    return pltpu.make_async_remote_copy(
        src_ref=src, dst_ref=dst, send_sem=sems[0].at[k], recv_sem=sems[1].at[k],
        device_id={"tp": to}, device_id_type=MESH)


def tail_kernel(side, n_dev, f_loc, v_loc, h_hbm, wg_hbm, wu_hbm, wd_hbm, gain, wv_hbm, temp, target, G, out,
                H, W, WD, X, WV, LT, ST, lsem, ssem, rsem, gssem, grsem, stsem, strsem):
    me, c, i, j, R1, L1, R2, L2, PT = place(side)
    rows, d = H.shape
    vpad = WV.shape[0]
    fpad = WD.shape[0]
    pieces = d // PIECE
    half = pieces // 2
    chunks = rows // CHUNK
    groups = rows // GROUP
    per = GROUP // CHUNK
    n1 = CHUNK // 2
    n2 = n1 // side
    f32 = lambda v: v.astype(jnp.float32)
    bf16 = lambda v: v.astype(jnp.bfloat16)
    nxt = lambda v: lax.rem(v + 1, side)
    prv = lambda v: lax.rem(v + side - 1, side)
    opp = lambda v: lax.rem(v + 2, side)

    loads = {}

    def load(name, src, dst):
        cp = pltpu.make_async_copy(src, dst, lsem.at[len(loads)])
        cp.start()
        loads[name] = cp

    for p in range(pieces):
        cols = pl.ds(p * PIECE, PIECE)
        load(("h", p), h_hbm.at[pl.ds(0, GROUP), cols], H.at[pl.ds(0, GROUP), cols])
        load(("g", p), wg_hbm.at[:, cols], W.at[pl.ds(0, f_loc), cols])
        load(("u", p), wu_hbm.at[:, cols], W.at[pl.ds(fpad, f_loc), cols])

    barrier = pltpu.get_barrier_semaphore()

    def greet(t, _):
        to = lax.rem(me + 1 + t, n_dev)
        pl.semaphore_signal(barrier, inc=1, device_id={"tp": to}, device_id_type=MESH)
        return 0
    lax.fori_loop(0, n_dev - 1, greet, 0)
    W[f_loc:fpad] = jnp.zeros((fpad - f_loc, d), W.dtype)
    W[fpad + f_loc:] = jnp.zeros((fpad - f_loc, d), W.dtype)
    WD[f_loc:] = jnp.zeros((fpad - f_loc, d), WD.dtype)
    WV[v_loc:] = jnp.zeros((vpad - v_loc, d), WV.dtype)

    sent, scratch_sent = [], [[] for _ in range(chunks)]

    def start(cp, scratch=None):
        cp.start()
        (sent if scratch is None else scratch_sent[scratch]).append(cp)
        return cp

    Y = G.at[0, 0]

    def mlp(b):
        cut = slice(b * GROUP, (b + 1) * GROUP)
        if b == 0:
            gu = None
            for p in range(pieces):
                for name in ("h", "g", "u"):
                    loads[name, p].wait()
                if p == pieces - 1:
                    load("wd", wd_hbm, WD.at[pl.ds(0, f_loc)])
                cols = slice(p * PIECE, (p + 1) * PIECE)
                more = lax.dot_general(W[:, cols], H[cut, cols], NT, preferred_element_type=jnp.float32)
                gu = more if gu is None else gu + more
            for q in range(1, rows // GROUP):
                load("h%d" % q, h_hbm.at[pl.ds(q * GROUP, GROUP)], H.at[pl.ds(q * GROUP, GROUP)])
            load("wv", wv_hbm, WV.at[pl.ds(0, v_loc)])
        else:
            loads["h%d" % b].wait()
            gu = lax.dot_general(W[...], H[cut], NT, preferred_element_type=jnp.float32)
        g, u = gu[:fpad], gu[fpad:]
        a = bf16((g * lax.logistic(g) * u).T)
        yield
        if b == 0:
            loads["wd"].wait()
        for p in range(pieces):
            Y[p, cut] = bf16(
                jnp.dot(a, WD[:, p * PIECE:(p + 1) * PIECE], preferred_element_type=jnp.float32))
            if b == 0 and p < BEFORE:
                continue
            if b == 0 and p == BEFORE:
                pl.semaphore_wait(barrier, n_dev - 1)
            for p2 in range(p + 1) if b == 0 and p == BEFORE else (p,):
                for q in range(b * per, (b + 1) * per):
                    theirs = Y.at[p2, pl.ds(pl.multiple_of(q * CHUNK + (1 - c) * n1, n1), n1)]
                    start(remote(theirs, G.at[0, 1, p2, pl.ds(q * CHUNK, n1)], (ssem, rsem), 26 * q + p2, PT), q)

    def chain(b):
        sems = (ssem, rsem)
        k0 = 26 * b
        P0 = G.at[0, 1]
        T = G.at[1, 0]
        lo, hi, every = pl.ds(0, half), pl.ds(half, half), pl.ds(0, pieces)
        row1 = lambda g: pl.multiple_of(b * CHUNK + c * n1 + g * n2, n2)

        def add_partner(g):
            at = pl.ds(row1(g), n2)
            frm = pl.ds(pl.multiple_of(b * CHUNK + g * n2, n2), n2)
            for p in range(pieces):
                Y[p, at] = bf16(f32(Y[p, at]) + f32(P0[p, frm]))

        def ring_sum(pos, row, n, R, L, t0, k, prepare):
            ta, tl, tr = pl.ds(t0, n), pl.ds(t0 + n, n), pl.ds(t0 + 2 * n, n)
            prepare(opp(pos))
            far = pl.ds(row(opp(pos)), n)
            right, left = pl.ds(row(nxt(pos)), n), pl.ds(row(prv(pos)), n)
            m0 = start(remote(Y.at[lo, far], T.at[lo, ta], sems, k, R), b)
            m1 = start(remote(Y.at[hi, far], T.at[hi, ta], sems, k + 1, L), b)
            prepare(nxt(pos))
            m2 = start(remote(Y.at[hi, right], T.at[hi, tl], sems, k + 2, R), b)
            prepare(prv(pos))
            m3 = start(remote(Y.at[lo, left], T.at[lo, tr], sems, k + 3, L), b)
            yield
            m0.wait_recv()
            for p in range(half):
                Y[p, right] = bf16(f32(Y[p, right]) + f32(T[p, ta]))
            m4 = start(remote(Y.at[lo, right], T.at[lo, tl], sems, k + 4, R), b)
            m1.wait_recv()
            for p in range(half, pieces):
                Y[p, left] = bf16(f32(Y[p, left]) + f32(T[p, ta]))
            m5 = start(remote(Y.at[hi, left], T.at[hi, tr], sems, k + 5, L), b)
            prepare(pos)
            yield
            for m in (m2, m3, m4, m5):
                m.wait_recv()
            own = pl.ds(row(pos), n)
            for p in range(pieces):
                total = f32(Y[p, own]) + f32(T[p, tl]) + f32(T[p, tr])
                yield p, total

        def drive(steps, keep):
            for got in steps:
                if got is None:
                    yield
                else:
                    keep(*got)

        yield
        for p in range(pieces):
            box = G.at[0, 1, p, pl.ds(b * CHUNK, n1)]
            remote(box, box, sems, k0 + p, PT).wait_recv()
        own1 = pl.ds(row1(i), n2)
        slot = lambda q: pl.ds(pl.multiple_of(b * CHUNK + side * n2 + q * n2, n2), n2)

        def keep1(p, total):
            T[p, slot(j)] = bf16(total)
        yield from drive(ring_sum(i, row1, n2, R1, L1, b * CHUNK, k0 + 4, add_partner), keep1)

        at = lambda ps, q: T.at[ps, slot(q)]
        for q, (ps, to) in enumerate(((lo, R2), (hi, L2), (hi, R2), (lo, L2))):
            start(remote(at(ps, j), at(ps, j), sems, k0 + 10 + q, to), b)
        yield
        remote(at(lo, prv(j)), at(lo, prv(j)), sems, k0 + 10, R2).wait_recv()
        start(remote(at(lo, prv(j)), at(lo, prv(j)), sems, k0 + 14, R2), b)
        remote(at(hi, nxt(j)), at(hi, nxt(j)), sems, k0 + 11, L2).wait_recv()
        start(remote(at(hi, nxt(j)), at(hi, nxt(j)), sems, k0 + 15, L2), b)
        yield
        for q, ps, frm in ((12, hi, prv(j)), (13, lo, nxt(j)), (14, lo, opp(j)), (15, hi, opp(j))):
            remote(at(ps, frm), at(ps, frm), sems, k0 + q, R2).wait_recv()
        sums = []
        square = jnp.zeros((n2, 1), jnp.float32)
        for p in range(pieces):
            y = f32(T[p, slot(0)])
            for q in range(1, side):
                y += f32(T[p, slot(q)])
            r = f32(H[own1, p * PIECE:(p + 1) * PIECE]) + y
            sums.append(r)
            square += jnp.sum(r * r, axis=-1, keepdims=True)
        inv = lax.rsqrt(square / d + NORM_EPS)
        for p in range(pieces):
            cols = slice(p * PIECE, (p + 1) * PIECE)
            X[own1, cols] = bf16(gain[0:1, cols] * sums[p] * inv)

        left_half, right_half = pl.ds(0, d // 2), pl.ds(d // 2, d // 2)

        at = lambda g, cols=pl.ds(0, d): X.at[pl.ds(row1(g), n2), cols]
        for q, (cols, to) in enumerate(((left_half, R1), (right_half, L1), (right_half, R1), (left_half, L1))):
            start(remote(at(i, cols), at(i, cols), sems, k0 + 16 + q, to))
        start(remote(at(i), at(i), sems, k0 + 22, PT))
        yield
        left, right, far = prv(i), nxt(i), opp(i)
        remote(at(left, left_half), at(left, left_half), sems, k0 + 16, R1).wait_recv()
        start(remote(at(left, left_half), at(left, left_half), sems, k0 + 20, R1))
        remote(at(right, right_half), at(right, right_half), sems, k0 + 17, L1).wait_recv()
        start(remote(at(right, right_half), at(right, right_half), sems, k0 + 21, L1))
        remote(at(left, right_half), at(left, right_half), sems, k0 + 18, R1).wait_recv()
        start(remote(at(left), at(left), sems, k0 + 23, PT))
        remote(at(right, left_half), at(right, left_half), sems, k0 + 19, L1).wait_recv()
        start(remote(at(right), at(right), sems, k0 + 24, PT))
        yield
        remote(at(far, left_half), at(far, left_half), sems, k0 + 20, R1).wait_recv()
        remote(at(far, right_half), at(far, right_half), sems, k0 + 21, L1).wait_recv()
        start(remote(at(far), at(far), sems, k0 + 25, PT))
        yield
        for q, g in enumerate((j, prv(j), nxt(j), opp(j))):
            line = X.at[pl.ds(pl.multiple_of(b * CHUNK + (1 - c) * n1 + g * n2, n2), n2)]
            remote(line, line, sems, k0 + 22 + q, PT).wait_recv()

    vid = lax.broadcasted_iota(jnp.int32, (vpad, GROUP), 0)

    def logits(b):
        cols = slice(b * GROUP, (b + 1) * GROUP)
        l = lax.dot_general(WV[...], X[cols], NT, preferred_element_type=jnp.float32) / temp[0:1, cols]
        LT[b] = l
        real = vid < v_loc
        m = jnp.max(jnp.where(real, l, -jnp.inf), axis=0, keepdims=True)
        e = jnp.where(real, jnp.exp(l - m), 0.0)
        s = jnp.sum(e, axis=0, keepdims=True)
        w = jnp.sum(e * l, axis=0, keepdims=True)
        ids = target[0:1, cols] - me * v_loc
        t = jnp.sum(jnp.where((vid == ids) & real, l, 0.0), axis=0, keepdims=True)
        both = [v[:, h * CHUNK:(h + 1) * CHUNK] for h in range(per) for v in (m, s, w, t)]
        ST[b, me] = jnp.concatenate(both, axis=0)
        for q in range(b * per, (b + 1) * per):
            for cp in scratch_sent[q]:
                cp.wait_send()
        tell(b)

    def tell(b):
        def body(t, _):
            to = lax.rem(me + 1 + t, n_dev)
            pltpu.make_async_remote_copy(
                src_ref=ST.at[b, me], dst_ref=ST.at[b, me], send_sem=stsem.at[b, t], recv_sem=strsem.at[b, t],
                device_id={"tp": to}, device_id_type=MESH).start()
            return 0
        lax.fori_loop(0, n_dev - 1, body, 0, unroll=True)

    def heard(b, wait):
        def body(t, _):
            frm = lax.rem(me + n_dev - 1 - t, n_dev)
            cp = pltpu.make_async_remote_copy(
                src_ref=ST.at[b, me], dst_ref=ST.at[b, frm], send_sem=stsem.at[b, t], recv_sem=strsem.at[b, t],
                device_id={"tp": frm}, device_id_type=MESH)
            wait(cp)
            return 0
        lax.fori_loop(0, n_dev - 1, body, 0, unroll=True)

    sems = (gssem, grsem)

    def blk(a, k, part):
        return G.at[c, a, j, pl.ds(k * CHUNK + part * (CHUNK // 2), CHUNK // 2)]

    def line(b, k):
        return G.at[c, :, b, pl.ds(k * CHUNK, CHUNK)]

    def one_of(a, b, k):
        return G.at[c, a, b, pl.ds(k * CHUNK, CHUNK)]

    def move(ref, k, q, to):
        start(remote(ref, ref, sems, 25 * k + q, to))

    def got(ref, k, q):
        remote(ref, ref, sems, 25 * k + q, PT).wait_recv()

    def combine(b):
        group, part = b // per, b % per
        if part == 0:
            heard(group, lambda cp: cp.wait_recv())
        st = ST[group]
        ms, ss, ws, ts = (st[:, q:q + 1, :] for q in range(4 * part, 4 * part + 4))
        m = jnp.max(ms, axis=0)
        f = jnp.exp(ms - m[None])
        s = jnp.sum(ss * f, axis=0)
        w = jnp.sum(ws * f, axis=0)
        t = jnp.sum(ts, axis=0)
        ln = m + jnp.log(s)
        cols = pl.ds(b * CHUNK, CHUNK)
        out[0:1, cols] = ln
        out[1:2, cols] = ln - w / s
        out[2:3, cols] = t - ln

        for v in range(0, vpad, 128):
            v = slice(v, v + 128)
            G[c, i, j, cols, v] = bf16((LT[group, v, part * CHUNK:(part + 1) * CHUNK] - ln).T)
        for q, (bit, to) in enumerate(((0, R1), (1, L1), (1, R1), (0, L1))):
            move(blk(i, b, bit), b, q, to)

    def first(k):
        left, right = prv(i), nxt(i)
        got(blk(left, k, 0), k, 0)
        move(blk(left, k, 0), k, 4, R1)
        got(blk(right, k, 1), k, 1)
        move(blk(right, k, 1), k, 5, L1)

    OWN, LEFT, RIGHT, FAR = range(4)
    stand = (i, prv(i), nxt(i), opp(i))

    def send(k, z, right=True, left=True):
        b = one_of(stand[z], j, k)
        if right:
            move(b, k, 6 + z, R2)
        if left:
            move(b, k, 10 + z, L2)

    def sides(k):
        got(blk(prv(i), k, 1), k, 2)
        got(blk(nxt(i), k, 0), k, 3)

    def far_side(k):
        got(blk(opp(i), k, 0), k, 4)
        got(blk(opp(i), k, 1), k, 5)

    def second(k):
        far_side(k)
        send(k, FAR)
        move(line(j, k), k, 18, PT)

    def third(k):
        for z, base, frm, sem, to in ((OWN, 6, prv(j), 14, R2), (LEFT, 10, nxt(j), 16, L2),
                                      (RIGHT, 6, prv(j), 15, R2), (FAR, 10, nxt(j), 17, L2)):
            b = one_of(stand[z], frm, k)
            got(b, k, base + z)
            move(b, k, sem, to)

    def fourth(k):
        for z in (LEFT, FAR):
            got(one_of(stand[z], prv(j), k), k, 6 + z)
        move(line(prv(j), k), k, 19, PT)
        for z in (OWN, RIGHT):
            got(one_of(stand[z], nxt(j), k), k, 10 + z)
        move(line(nxt(j), k), k, 20, PT)
        for z, sem in ((OWN, 14), (LEFT, 16), (RIGHT, 15), (FAR, 17)):
            b = one_of(stand[z], opp(j), k)
            got(b, k, sem)
            move(b, k, 21 + z, PT)

    def last(k):
        for q, g in enumerate((i, prv(i), nxt(i))):
            got(G.at[1 - c, :, g, pl.ds(k * CHUNK, CHUNK)], k, 18 + q)
        for z, a in enumerate((j, prv(j), nxt(j), opp(j))):
            got(G.at[1 - c, a, opp(i), pl.ds(k * CHUNK, CHUNK)], k, 21 + z)

    def lockstep(g):
        mine = [chain(b) for b in range(g * per, (g + 1) * per)]
        for one in mine:
            next(one)
        ended = False
        while not ended:
            for one in mine:
                ended = next(one, "end") == "end"
            if not ended:
                yield

    assert groups == 2 and per == 2
    for _ in mlp(0):
        pass
    one, two = lockstep(0), lockstep(1)
    next(one)
    for _ in mlp(1):
        next(one)
    loads["wv"].wait()
    rnd = 0
    while next(one, "end") != "end":
        rnd += 1
        if rnd > LAG:
            next(two)
    def both(k):
        sides(k)
        far_side(k)
        for zr, zl in ((OWN, LEFT), (RIGHT, FAR), (LEFT, OWN), (FAR, RIGHT)):
            send(k, zr, left=False)
            send(k, zl, right=False)
        move(line(j, k), k, 18, PT)

    logits(0)
    next(two)
    combine(0)
    send(0, OWN)
    combine(1)
    next(two, None)
    first(0)
    next(two, None)
    sides(0)
    send(0, LEFT)
    next(two, None)
    send(0, RIGHT)
    first(1)
    for _ in two:
        pass
    second(0)
    logits(1)
    third(0)
    both(1)
    combine(2)
    combine(3)
    for b in range(groups):
        heard(b, lambda cp: cp.wait_send())
    marks = [0] * SETTLE
    settled = 0
    for act, k in ((first, 2), (third, 1), (first, 3), (fourth, 0), (both, 2), (fourth, 1), (both, 3), (last, 0),
                   (third, 2), (last, 1), (third, 3), (fourth, 2), (last, 2), (fourth, 3), (last, 3)):
        upto = marks[-SETTLE]
        for cp in sent[settled:upto]:
            cp.wait_send()
        settled = max(settled, upto)
        marks.append(len(sent))
        act(k)
    for cp in sent[settled:]:
        cp.wait_send()


def layout_kernel(side, v_loc, g, o, stage, sem):
    slots, step, _ = stage.shape
    steps = o.shape[0] // step

    def out(s, slot):
        return pltpu.make_async_copy(stage.at[slot], o.at[pl.ds(pl.multiple_of(s * step, step), step)], sem.at[slot])

    def body(s, _):
        slot = lax.rem(s, slots)

        @pl.when(s >= slots)
        def _():
            out(s - slots, slot).wait()
        r = pl.ds(pl.multiple_of(s * step, step), step)
        for fam in range(2):
            for a in range(side):
                for b in range(side):
                    dev = ((b * side + a) * 2) if fam == 0 else ((a * side + b) * 2 + 1)
                    stage[slot, :, dev * v_loc:(dev + 1) * v_loc] = g[fam, a, b, r, 0:v_loc]
        out(s, slot).start()
        return 0
    lax.fori_loop(0, steps, body, 0)
    for s in range(steps - slots, steps):
        out(s, s % slots).wait()


def solution(mesh):
    n_dev = mesh.shape["tp"]
    side = math.isqrt(n_dev // 2)

    def device_step(hidden, w_gate, w_up, w_down, norm_gain, w_vocab, temperature, target):
        rows, d = hidden.shape
        f_loc, v_loc = w_gate.shape[1], w_vocab.shape[1]
        vpad = -(-v_loc // 128) * 128
        fpad = -(-f_loc // 128) * 128
        vm = pl.BlockSpec(memory_space=pltpu.VMEM)
        hbm = pl.BlockSpec(memory_space=pl.ANY)
        bf = jnp.bfloat16
        chunks, groups = rows // CHUNK, rows // GROUP
        dma = pltpu.SemaphoreType.DMA
        g, stats = pl.pallas_call(
            functools.partial(tail_kernel, side, n_dev, f_loc, v_loc),
            out_shape=(pltpu.VMEM((2, side, side, rows, vpad), bf), pltpu.VMEM((8, rows), jnp.float32)),
            in_specs=[hbm, hbm, hbm, hbm, vm, hbm, vm, vm],
            out_specs=(vm, vm),
            scratch_shapes=[
                pltpu.VMEM((rows, d), bf),
                pltpu.VMEM((2 * fpad, d), bf),
                pltpu.VMEM((fpad, d), bf),
                pltpu.VMEM((rows, d), bf),
                pltpu.VMEM((vpad, d), bf),
                pltpu.VMEM((groups, vpad, GROUP), jnp.float32),
                pltpu.VMEM((groups, n_dev, 8, CHUNK), jnp.float32),
                dma((3 * (d // PIECE) + groups + 1,)),
                dma((26 * chunks,)), dma((26 * chunks,)),
                dma((25 * chunks,)), dma((25 * chunks,)),
                dma((groups, n_dev - 1)), dma((groups, n_dev - 1)),
            ],
            compiler_params=pltpu.CompilerParams(
                collective_id=0, has_side_effects=True, vmem_limit_bytes=30 << 20),
            name="tail",
        )(hidden, w_gate.T, w_up.T, w_down, norm_gain.reshape(1, d), w_vocab.T, temperature.reshape(1, rows),
          target.reshape(1, rows))

        log_probs = pl.pallas_call(
            functools.partial(layout_kernel, side, v_loc),
            out_shape=jax.ShapeDtypeStruct((rows, n_dev * v_loc), bf),
            in_specs=[vm],
            out_specs=hbm,
            scratch_shapes=[pltpu.VMEM((4, 16, n_dev * v_loc), bf), dma((4,))],
            compiler_params=pltpu.CompilerParams(vmem_limit_bytes=16 << 20),
            name="layout",
        )(g)
        return stats[0], stats[1], stats[2], log_probs

    return jax.shard_map(
        device_step,
        mesh=mesh,
        in_specs=(P("dp", None), P(None, "tp"), P(None, "tp"), P("tp", None), P(None),
                  P(None, "tp"), P("dp"), P("dp")),
        out_specs=(P("dp"), P("dp"), P("dp"), P("dp", None)),
        check_vma=False,
    )
```
